256 devices in a mesh: gz: 16 (over x, y), gy: 16 (over z, core).
Axes of the slice: x: 4, y: 4, z: 8, core: 2. Of those that a mesh axis runs over, the one named last changes fastest.
Arguments:
- fixed: float32 [512, 1024, 256], P('gz', 'gy'), may hold values from -6 to 6
- moving: float32 [512, 1024, 256], P('gz', 'gy'), may hold values from -6 to 6
Outputs:
- update: float32 [3, 64, 128, 32], P(None, 'gz', 'gy')
- residual: float32 [3, 64, 128, 32], P(None, 'gz', 'gy')
The draws below stay inside these ranges and needn't reach their ends.
All inputs are finite; a program needn't handle non-finite values.
Results may differ from the reference program's by a relative error of at most 0.0031.
Values sent between devices are 32-bit elements; how exact they have to be, the bound alone decides.
A program may use at most 64 MiB of HBM per device.

```python
import jax
import jax.numpy as jnp
from jax import lax

SPACING = 8
ITERS = 2
CZ = 32
CY = 64
NX = 256
NZ = 512
NY = 1024
NCZ = 64
NCY = 128
NCX = 32
N_GZ = 16
N_GY = 16


def block_scale(stream_key, shape, shards, smallest, largest):
    level, own = 1.0, jax.random.fold_in(stream_key, 6)
    for axis_at, parts in shards:
        draws = jnp.exp(jax.random.uniform(jax.random.fold_in(own, axis_at), (parts,), jnp.float32, smallest / len(shards), largest / len(shards)))
        level = level * jnp.repeat(draws, shape[axis_at] // parts).reshape([-1 if axis == axis_at else 1 for axis in range(len(shape))])
    return level


def centred(rng, extent, deviation, reach, cuts=(), kind=jnp.bfloat16):
    result = deviation * jax.random.normal(rng, extent, jnp.float32)
    if cuts:
        result = result * block_scale(rng, extent, cuts, -0.22, 0.18)
    return jnp.clip(result, -reach, reach).astype(kind)


def setup_inputs(seed: int = 0) -> dict:
    key_list = jax.random.split(jax.random.key(seed), 3)
    fixed = centred(key_list[0], (NZ, NY, NX), 1.0, 6.0, ((0, 16), (1, 16)), jnp.float32)
    moving = centred(key_list[1], (NZ, NY, NX), 1.0, 6.0, ((0, 16), (1, 16)), jnp.float32)
    return {"fixed": fixed, "moving": moving}


damping_weight = 8.0


def basis_matrix(count, columns, offset):
    voxel = jnp.arange(count, dtype=jnp.int32)
    cell = voxel // SPACING
    frac = ((voxel % SPACING).astype(jnp.float32) + 0.5) / SPACING
    other = 1.0 - frac
    weights = (other ** 3 / 6.0, (3.0 * frac ** 3 - 6.0 * frac ** 2 + 4.0) / 6.0,
               (-3.0 * frac ** 3 + 3.0 * frac ** 2 + 3.0 * frac + 1.0) / 6.0, frac ** 3 / 6.0)
    index = jnp.arange(columns, dtype=jnp.int32)
    matrix = jnp.zeros((count, columns), jnp.float32)
    for tap in range(4):
        match = index[None, :] == (cell - 1 + tap + offset)[:, None]
        matrix = matrix + jnp.where(match, weights[tap][:, None], jnp.float32(0.0))
    return matrix


def decode(control, along_z, along_y, along_x):
    hp = lax.Precision.HIGHEST
    inner = jnp.einsum('cabe,xe->cabx', control, along_x, precision=hp)
    inner = jnp.einsum('yb,cabx->cayx', along_y, inner, precision=hp)
    return jnp.einsum('za,cayx->czyx', along_z, inner, precision=hp)


def encode(volume, along_z, along_y, along_x):
    hp = lax.Precision.HIGHEST
    inner = jnp.einsum('za,czyx->cayx', along_z, volume, precision=hp)
    inner = jnp.einsum('yb,cayx->cabx', along_y, inner, precision=hp)
    return jnp.einsum('xe,cabx->cabe', along_x, inner, precision=hp)


def derivative(padded, axis):
    length = padded.shape[axis] - 6

    def part(shift_by):
        return lax.slice_in_dim(padded, 3 + shift_by, 3 + shift_by + length, axis=axis)

    return (45.0 * (part(1) - part(-1)) - 9.0 * (part(2) - part(-2)) + (part(3) - part(-3))) / 60.0


def gradients(padded):
    return jnp.stack([derivative(padded[:, 3:-3, 3:-3], 0),
                      derivative(padded[3:-3, :, 3:-3], 1),
                      derivative(padded[3:-3, 3:-3, :], 2)])


def reference(fixed, moving):
    mean = 0.5 * (fixed + moving)
    gradient = gradients(jnp.pad(mean, 3)).astype(jnp.bfloat16)
    mismatch = moving - fixed
    ctrl_z = CZ // SPACING
    ctrl_y = CY // SPACING
    ctrl_x = NX // SPACING
    along_z = basis_matrix(CZ, ctrl_z + 4, 2)
    along_y = basis_matrix(CY, ctrl_y + 4, 2)
    along_x = basis_matrix(NX, ctrl_x, 0)
    zero = jnp.int32(0)

    def accumulate(control, with_data):
        padded = jnp.pad(control, ((0, 0), (2, 2), (2, 2), (0, 0)))

        def step(total, block):
            zb = block // N_GY
            yb = block % N_GY
            slab = lax.dynamic_slice(gradient, (zero, zb * CZ, yb * CY, zero), (3, CZ, CY, NX)).astype(jnp.float32)
            start = (zero, zb * ctrl_z, yb * ctrl_y, zero)
            shape = (3, ctrl_z + 4, ctrl_y + 4, ctrl_x)
            if with_data:
                local = lax.dynamic_slice(mismatch, (zb * CZ, yb * CY, zero), (CZ, CY, NX))
                volume = slab * local[None]
            else:
                field = decode(lax.dynamic_slice(padded, start, shape), along_z, along_y, along_x)
                volume = slab * jnp.sum(slab * field, axis=0)[None]
            back = encode(volume, along_z, along_y, along_x)
            current = lax.dynamic_slice(total, start, shape)
            return lax.dynamic_update_slice(total, current + back, start), None

        total, unused = lax.scan(step, jnp.zeros_like(padded), jnp.arange(N_GZ * N_GY, dtype=jnp.int32))
        return total[:, 2:-2, 2:-2, :]

    shape = (3, NCZ, NCY, NCX)
    rhs = -accumulate(jnp.zeros(shape, jnp.float32), True)
    update = jnp.zeros(shape, jnp.float32)
    residual = rhs
    direction = rhs
    norm_now = jnp.sum(residual * residual)
    for step_index in range(ITERS):
        image = accumulate(direction, False) + damping_weight * direction
        alpha = norm_now / jnp.sum(direction * image)
        update = update + alpha * direction
        residual = residual - alpha * image
        norm_next = jnp.sum(residual * residual)
        direction = residual + (norm_next / norm_now) * direction
        norm_now = norm_next
    return update, residual
```

```python
import functools

import jax
import jax.numpy as jnp
import numpy as np
from jax import lax
from jax.experimental import pallas as pl
from jax.experimental.pallas import tpu as pltpu
from jax.sharding import PartitionSpec as P

SPACING = 8
DAMPING = 8.0
CZ, CY, NX = 32, 64, 256
CA, CB, CE = 4, 8, 32
A, B, LANES = 7, 16, 128
BP = 12
ROWS = A * BP
CHUNK = 256
STEPS = CZ * CY // CHUNK
MESH = pl.DeviceIdType.MESH
F32, BF16 = jnp.float32, jnp.bfloat16


def basis_matrix(count, columns, offset):
    voxel = np.arange(count)
    cell = voxel // SPACING
    frac = (voxel % SPACING + 0.5) / SPACING
    other = 1.0 - frac
    weights = (
        other**3 / 6.0,
        (3.0 * frac**3 - 6.0 * frac**2 + 4.0) / 6.0,
        (-3.0 * frac**3 + 3.0 * frac**2 + 3.0 * frac + 1.0) / 6.0,
        frac**3 / 6.0,
    )
    matrix = np.zeros((count, columns))
    for tap in range(4):
        for v in range(count):
            column = cell[v] - 1 + tap + offset
            if 0 <= column < columns:
                matrix[v, column] += weights[tap][v]
    return matrix


def halves(x):
    x = np.asarray(x, np.float32)
    high = x.astype(jnp.bfloat16)
    low = (x - high.astype(np.float32)).astype(jnp.bfloat16)
    return high, low


def constants():
    bz = basis_matrix(CZ, A, 1)
    by = basis_matrix(CY, B, 1)
    bx = basis_matrix(NX, CE, 0)
    kron12 = np.einsum("za,yb->zyab", bz, by[:, :BP]).reshape(CZ * CY, ROWS)
    high, low = halves(kron12)
    pad = np.zeros((CZ * CY, 256 - 3 * ROWS), jnp.bfloat16)
    kd = np.concatenate([high, high, low, pad], axis=1)
    kron16 = np.einsum("za,yb->abzy", bz, by).reshape(A * B, CZ * CY)
    ke = np.concatenate(halves(kron16), axis=0)
    spread = np.zeros((LANES, 3 * NX))
    for c in range(3):
        spread[c * CE : (c + 1) * CE, c * NX : (c + 1) * NX] = bx.T
    high, low = halves(spread)
    bxd = np.concatenate([high, high, low], axis=0)
    gather = np.concatenate([high.T, low.T], axis=1)
    bxe = np.concatenate([gather, gather], axis=0)
    dx = np.zeros((NX, NX))
    for step, weight in ((1, 45.0), (2, -9.0), (3, 1.0)):
        for v in range(NX):
            if v + step < NX:
                dx[v + step, v] = weight
            if v - step >= 0:
                dx[v - step, v] = -weight
    dx = np.concatenate([dx, dx], axis=0).astype(jnp.bfloat16)
    return kd, ke, bxd, bxe, dx


def split(x):
    high = x.astype(BF16)
    return high, (x - high.astype(F32)).astype(BF16)


def dot(a, b):
    return jnp.dot(a, b, preferred_element_type=F32)


def kernel(nz, ny, fixed, moving, kd_h, ke_h, bxd_h, bxe_h, dx_h, upd, res,
           fv, mv, mp, fl, ml, fh, mh, yls, yhs, zlr, zhr, ylr, yhr,
           g, s0, sw, u, cs, p3, kd, ke, bxd, bxe, dx,
           enc, rz, ry, rc, ars, arr,
           lsem, hss, hrs, xss, xrs, ass, arsem):
    d = lax.axis_index("gz")
    e = lax.axis_index("gy")
    up, down = lax.rem(d + 1, nz), lax.rem(d + nz - 1, nz)
    right, left = lax.rem(e + 1, ny), lax.rem(e + ny - 1, ny)

    barrier = pltpu.get_barrier_semaphore()

    def greet_y(k, carry):
        pl.semaphore_signal(barrier, inc=1, device_id=(d, lax.rem(e + k, ny)), device_id_type=MESH)
        return carry

    def greet_z(k, carry):
        pl.semaphore_signal(barrier, inc=1, device_id=(lax.rem(d + k, nz), e), device_id_type=MESH)
        return carry

    for z in (up, down):
        for y in (right, left):
            pl.semaphore_signal(barrier, inc=1, device_id=(z, y), device_id_type=MESH)
    lax.fori_loop(1, ny, greet_y, 0)
    lax.fori_loop(1, nz, greet_z, 0)

    def local(k, src, dst):
        copy = pltpu.make_async_copy(src, dst, lsem.at[k])
        copy.start()
        return copy

    faces_z = [
        local(0, fixed.at[pl.ds(0, 3)], fv.at[pl.ds(0, 3)]),
        local(1, moving.at[pl.ds(0, 3)], mv.at[pl.ds(0, 3)]),
        local(2, fixed.at[pl.ds(CZ - 3, 3)], fv.at[pl.ds(CZ - 3, 3)]),
        local(3, moving.at[pl.ds(CZ - 3, 3)], mv.at[pl.ds(CZ - 3, 3)]),
    ]
    faces_y = [
        local(4, fixed.at[:, pl.ds(0, 8)], fl),
        local(5, moving.at[:, pl.ds(0, 8)], ml),
        local(6, fixed.at[:, pl.ds(CY - 8, 8)], fh),
        local(7, moving.at[:, pl.ds(CY - 8, 8)], mh),
    ]
    rest = [
        local(8, fixed.at[pl.ds(3, CZ - 6)], fv.at[pl.ds(3, CZ - 6)]),
        local(9, moving.at[pl.ds(3, CZ - 6)], mv.at[pl.ds(3, CZ - 6)]),
        local(10, dx_h, dx),
        local(11, bxe_h, bxe),
    ]
    later = [local(12, ke_h, ke), local(13, bxd_h, bxd), local(14, kd_h, kd)]

    def remote(src, dst, send, recv, z, y):
        return pltpu.make_async_remote_copy(
            src_ref=src, dst_ref=dst, send_sem=send, recv_sem=recv, device_id=(z, y), device_id_type=MESH
        )

    for copy in faces_z:
        copy.wait()
    for z in (0, 1, 2, CZ - 3, CZ - 2, CZ - 1):
        mp[z + 3, 8 : 8 + CY, :] = 0.5 * (fv[z] + mv[z])
    for copy in faces_y:
        copy.wait()
    yls[...] = 0.5 * (fl[:, 0:4, :] + ml[:, 0:4, :])
    yhs[...] = 0.5 * (fh[:, 4:8, :] + mh[:, 4:8, :])
    pl.semaphore_wait(barrier, 4 + (ny - 1) + (nz - 1))
    halo = [
        remote(mp.at[pl.ds(CZ, 3), pl.ds(8, CY)], zlr, hss.at[0], hrs.at[0], up, e),
        remote(mp.at[pl.ds(3, 3), pl.ds(8, CY)], zhr, hss.at[1], hrs.at[1], down, e),
        remote(yhs, ylr, hss.at[2], hrs.at[2], d, right),
        remote(yls, yhr, hss.at[3], hrs.at[3], d, left),
    ]
    for copy in halo:
        copy.start()

    has_down = jnp.where(d > 0, 1.0, 0.0).astype(F32)
    has_up = jnp.where(d < nz - 1, 1.0, 0.0).astype(F32)
    has_left = jnp.where(e > 0, 1.0, 0.0).astype(F32)
    has_right = jnp.where(e < ny - 1, 1.0, 0.0).astype(F32)
    p3[...] = jnp.zeros_like(p3)

    for copy in rest:
        copy.wait()

    def fill(z, carry):
        mp[z + 3, 8 : 8 + CY, :] = 0.5 * (fv[z] + mv[z])
        return carry

    lax.fori_loop(3, CZ - 3, fill, 0)

    halo[2].wait_recv()
    mp[3 : CZ + 3, 4:8, :] = has_left * ylr[...]
    halo[3].wait_recv()
    mp[3 : CZ + 3, 8 + CY : 12 + CY, :] = has_right * yhr[...]

    def gather_x(volume, j):
        parts = [split(v) for v in volume]
        total = None
        for c in range(3):
            weights = bxe[pl.ds(c * NX, NX), :]
            for part in parts[c]:
                term = dot(part, weights)
                total = term if total is None else total + term
        high, low = split(total[:, :LANES] + total[:, LANES:])
        rows = pl.ds(pl.multiple_of(j * CHUNK, CHUNK), CHUNK)
        u[rows, 0:LANES] = high
        u[rows, LANES : 2 * LANES] = low

    def first(j):
        z = j * 4
        rows = pl.ds(pl.multiple_of(j * CHUNK, CHUNK), CHUNK)

        def along_z(k):
            return mp[pl.ds(z + 3 + k, 4), 8 : 8 + CY, :]

        def along_y(k):
            return mp[pl.ds(z + 3, 4), 8 + k : 8 + k + CY, :]

        def difference(part):
            return 45.0 * (part(1) - part(-1)) - 9.0 * (part(2) - part(-2)) + (part(3) - part(-3))

        centre = along_z(0).reshape(CHUNK, NX)
        high, low = split(centre)
        sixtieth = 1.0 / 60.0
        slopes = (
            difference(along_z).reshape(CHUNK, NX),
            difference(along_y).reshape(CHUNK, NX),
            dot(high, dx[0:NX, :]) + dot(low, dx[NX : 2 * NX, :]),
        )
        mismatch = (fv[pl.ds(z, 4)] - mv[pl.ds(z, 4)]).reshape(CHUNK, NX)
        volume = []
        for c in range(3):
            rounded = (slopes[c] * sixtieth).astype(BF16)
            g[c, rows, :] = rounded
            volume.append(rounded.astype(F32) * mismatch)
        gather_x(volume, j)

    def first_inner(j, carry):
        first(j)
        return carry

    lax.fori_loop(1, STEPS - 1, first_inner, 0)
    halo[0].wait_recv()
    mp[0:3, 8 : 8 + CY, :] = has_down * zlr[...]
    halo[1].wait_recv()
    mp[CZ + 3 : CZ + 6, 8 : 8 + CY, :] = has_up * zhr[...]

    def first_outer(t, carry):
        first(t * (STEPS - 1))
        return carry

    lax.fori_loop(0, 2, first_outer, 0)
    for copy in later:
        copy.wait()

    row = lax.broadcasted_iota(jnp.int32, (1, 8, LANES), 1)
    low_rows = jnp.where(row < 3, 1.0, 0.0).astype(F32)
    from_right = has_right * low_rows
    pa = lax.broadcasted_iota(jnp.int32, (A, B, LANES), 0) + (d * CA - 1)
    pb = lax.broadcasted_iota(jnp.int32, (A, B, LANES), 1) + (e * CB - 1)
    ia = lax.broadcasted_iota(jnp.int32, (A, B, LANES), 0)
    ib = lax.broadcasted_iota(jnp.int32, (A, B, LANES), 1)
    inside = (pa >= 0) & (pa < nz * CA) & (pb >= 0) & (pb < ny * CB) & (ib < 11)
    inside = jnp.where(inside, 1.0, 0.0).astype(F32)
    own = jnp.where((ia >= 1) & (ia < 1 + CA) & (ib >= 1) & (ib < 1 + CB), 1.0, 0.0).astype(F32)

    def exchange(k):
        both = dot(ke[...], u[...])
        half = A * B
        total = both[:half, :LANES] + both[half:, :LANES] + both[:half, LANES:]
        enc[k] = total.reshape(A, B, LANES)
        src = enc.at[k]
        top, bottom = pl.ds(A - 3, 3), pl.ds(0, 3)
        after, before = pl.ds(8, 8), pl.ds(0, 8)
        copies = [
            remote(src.at[top, after], rc.at[k, 0], xss.at[k, 0], xrs.at[k, 0], up, right),
            remote(src.at[top, before], rc.at[k, 1], xss.at[k, 1], xrs.at[k, 1], up, left),
            remote(src.at[bottom, after], rc.at[k, 2], xss.at[k, 2], xrs.at[k, 2], down, right),
            remote(src.at[bottom, before], rc.at[k, 3], xss.at[k, 3], xrs.at[k, 3], down, left),
            remote(src.at[top], rz.at[k, 0], xss.at[k, 4], xrs.at[k, 4], up, e),
            remote(src.at[bottom], rz.at[k, 1], xss.at[k, 5], xrs.at[k, 5], down, e),
            remote(src.at[:, after], ry.at[k, 0], xss.at[k, 6], xrs.at[k, 6], d, right),
            remote(src.at[:, before], ry.at[k, 1], xss.at[k, 7], xrs.at[k, 7], d, left),
        ]
        for copy in copies:
            copy.start()
        return copies

    def collect(k, copies):
        for copy in copies:
            copy.wait_recv()
        left_half = enc[k, :, 0:8, :] + has_left * ry[k, 0]
        right_half = enc[k, :, 8:16, :] + from_right * ry[k, 1]
        below = has_down * rz[k, 0]
        above = has_up * rz[k, 1]
        left_low = below[:, 0:8] + (has_down * has_left) * rc[k, 0]
        right_low = below[:, 8:16] + has_down * from_right * rc[k, 1]
        left_high = above[:, 0:8] + (has_up * has_left) * rc[k, 2]
        right_high = above[:, 8:16] + has_up * from_right * rc[k, 3]

        def stack(middle, low, high):
            return jnp.concatenate([middle[0:3] + low, middle[3:4], middle[4:7] + high], axis=0)

        whole = jnp.concatenate(
            [stack(left_half, left_low, left_high), stack(right_half, right_low, right_high)], axis=1
        )
        return whole * inside

    def spread_x(control):
        for t in range(3):
            for a in range(A):
                p3[t * ROWS + a * BP : t * ROWS + (a + 1) * BP, :] = control[a, 0:BP, :]
        high, low = split(p3[...])
        wide = dot(jnp.concatenate([high, low, high], axis=1), bxd[...])
        index = lax.broadcasted_iota(jnp.int32, (256, 3 * NX), 0)
        middle = (index >= ROWS) & (index < 2 * ROWS)
        rounded = wide.astype(BF16).astype(F32)
        cs[...] = jnp.where(middle, wide - rounded, rounded).astype(BF16)

    def apply(dst, j, carry):
        rows = pl.ds(pl.multiple_of(j * CHUNK, CHUNK), CHUNK)
        field = dot(kd[rows, :], cs[...])
        slopes = [g[c, rows, :].astype(F32) for c in range(3)]
        s = slopes[0] * field[:, 0:NX]
        s = s + slopes[1] * field[:, NX : 2 * NX]
        s = s + slopes[2] * field[:, 2 * NX : 3 * NX]
        dst[rows, :] = s
        gather_x([slopes[c] * s for c in range(3)], j)
        return carry + jnp.sum((s * s).reshape(CHUNK // 8, 8, NX), axis=0)

    def fold(x):
        total = jnp.sum(x, axis=0, keepdims=True)
        return total[:, 0:LANES] + total[:, LANES : 2 * LANES]

    def tile_sum(x):
        return jnp.sum(jnp.sum(x, axis=0), axis=0, keepdims=True)

    def reduce_start(i, stage, value):
        me, count = (e, ny) if stage == 0 else (d, nz)
        ars[i, stage] = value
        arr[i, stage, me] = value

        def send(k, carry):
            other = lax.rem(me + k, count)
            z, y = (d, other) if stage == 0 else (other, e)
            remote(ars.at[i, stage], arr.at[i, stage, me], ass.at[i, stage, k], arsem.at[i, stage, me], z, y).start()
            return carry

        lax.fori_loop(1, count, send, 0)

    def reduce_end(i, stage):
        me, count = (e, ny) if stage == 0 else (d, nz)

        def take(k, carry):
            other = lax.rem(me + count - k, count)
            remote(ars.at[i, stage], arr.at[i, stage, other], ass.at[i, stage, k], arsem.at[i, stage, other], d, e).wait_recv()
            return carry

        lax.fori_loop(1, count, take, 0)
        return jnp.sum(arr[i, stage], axis=0)

    def scalars(i):
        total = reduce_end(i, 1)
        total = jnp.sum(total, axis=1, keepdims=True)
        return total[0:1], total[1:2]

    copies0 = exchange(0)
    r0 = collect(0, copies0)
    spread_x(r0)
    square = tile_sum(r0 * r0 * own)
    zero = jnp.zeros((8, NX), F32)
    energy = fold(lax.fori_loop(0, STEPS, functools.partial(apply, s0), zero))
    copies1 = exchange(1)
    reduce_start(0, 0, jnp.concatenate([square, energy], axis=0))
    w0 = collect(1, copies1) + DAMPING * r0
    reduce_start(0, 1, reduce_end(0, 0))
    spread_x(w0)
    lax.fori_loop(0, STEPS, functools.partial(apply, sw), zero)
    copies2 = exchange(2)
    rr0, energy0 = scalars(0)
    alpha0 = rr0 / (energy0 + DAMPING * rr0)
    r1 = r0 - alpha0.reshape(1, 1, 1) * w0

    def combine(j, carry):
        rows = pl.ds(pl.multiple_of(j * CHUNK, CHUNK), CHUNK)
        s = s0[rows, :] - alpha0 * sw[rows, :]
        return carry + jnp.sum((s * s).reshape(CHUNK // 8, 8, NX), axis=0)

    energy = fold(lax.fori_loop(0, STEPS, combine, zero))
    reduce_start(1, 0, jnp.concatenate([tile_sum(r1 * r1 * own), energy], axis=0))
    v = collect(2, copies2) + DAMPING * w0
    reduce_start(1, 1, reduce_end(1, 0))
    rr1, energy1 = scalars(1)
    beta = rr1 / rr0
    product = energy1 + DAMPING * rr1 - beta * rr1 / alpha0
    alpha1 = rr1 / product
    alpha0, alpha1, beta = (x.reshape(1, 1, 1) for x in (alpha0, alpha1, beta))
    direction = r1 + beta * r0
    along = w0 - alpha0 * v + beta * w0
    update = alpha0 * r0 + alpha1 * direction
    residual = r1 - alpha1 * along
    for c in range(3):
        upd[c] = update[1 : 1 + CA, 1 : 1 + CB, c * CE : (c + 1) * CE]
        res[c] = residual[1 : 1 + CA, 1 : 1 + CB, c * CE : (c + 1) * CE]

    for copy in halo + copies0 + copies1 + copies2:
        copy.wait_send()
    for i in range(2):
        for stage in range(2):
            count = ny if stage == 0 else nz

            def sent(k, carry):
                remote(ars.at[i, stage], arr.at[i, stage, 0], ass.at[i, stage, k], arsem.at[i, stage, 0], d, e).wait_send()
                return carry

            lax.fori_loop(1, count, sent, 0)


def solution(mesh):
    nz, ny = mesh.shape["gz"], mesh.shape["gy"]
    tables = constants()
    count = max(nz, ny)
    vmem = pltpu.VMEM
    dma = pltpu.SemaphoreType.DMA
    scratch = [
        vmem((CZ, CY, NX), F32), vmem((CZ, CY, NX), F32),
        vmem((CZ + 6, CY + 16, NX), F32),
        vmem((CZ, 8, NX), F32), vmem((CZ, 8, NX), F32), vmem((CZ, 8, NX), F32), vmem((CZ, 8, NX), F32),
        vmem((CZ, 4, NX), F32), vmem((CZ, 4, NX), F32),
        vmem((3, CY, NX), F32), vmem((3, CY, NX), F32),
        vmem((CZ, 4, NX), F32), vmem((CZ, 4, NX), F32),
        vmem((3, CZ * CY, NX), BF16),
        vmem((CZ * CY, NX), F32), vmem((CZ * CY, NX), F32),
        vmem((CZ * CY, 2 * LANES), BF16),
        vmem((256, 3 * NX), BF16),
        vmem((256, LANES), F32),
    ] + [vmem(t.shape, BF16) for t in tables] + [
        vmem((3, A, B, LANES), F32),
        vmem((3, 2, 3, B, LANES), F32),
        vmem((3, 2, A, 8, LANES), F32),
        vmem((3, 4, 3, 8, LANES), F32),
        vmem((2, 2, 2, LANES), F32),
        vmem((2, 2, count, 2, LANES), F32),
        dma((15,)), dma((4,)), dma((4,)), dma((3, 8)), dma((3, 8)), dma((2, 2, count)), dma((2, 2, count)),
    ]
    out = jax.ShapeDtypeStruct((3, CA, CB, CE), F32)
    call = pl.pallas_call(
        functools.partial(kernel, nz, ny),
        out_shape=(out, out),
        in_specs=[pl.BlockSpec(memory_space=pl.ANY)] * 7,
        out_specs=(pl.BlockSpec(memory_space=pltpu.VMEM), pl.BlockSpec(memory_space=pltpu.VMEM)),
        scratch_shapes=scratch,
        compiler_params=pltpu.CompilerParams(collective_id=0, has_side_effects=True, vmem_limit_bytes=56 * 1024 * 1024),
        name="cg_step",
    )

    def shards(fixed, moving):
        return call(fixed, moving, *[jnp.asarray(t) for t in tables])

    return jax.shard_map(
        shards,
        mesh=mesh,
        in_specs=(P("gz", "gy", None), P("gz", "gy", None)),
        out_specs=(P(None, "gz", "gy", None), P(None, "gz", "gy", None)),
        check_vma=False,
    )
```

```python
import functools

import jax
import jax.numpy as jnp
import numpy as np
from jax import lax
from jax.experimental import pallas as pl
from jax.experimental.pallas import tpu as pltpu
from jax.sharding import PartitionSpec as P

SPACING = 8
DAMPING = 8.0
CZ, CY, NX = 32, 64, 256
CA, CB, CE = 4, 8, 32
A, B, LANES = 7, 16, 128
BP = 12
ROWS = A * BP
CHUNK = 1024
STEPS = CZ * CY // CHUNK
INNER = 8
OUTER = 4
MESH = pl.DeviceIdType.MESH
F32, BF16 = jnp.float32, jnp.bfloat16


def basis_matrix(count, columns, offset):
    voxel = np.arange(count)
    cell = voxel // SPACING
    frac = (voxel % SPACING + 0.5) / SPACING
    other = 1.0 - frac
    weights = (
        other**3 / 6.0,
        (3.0 * frac**3 - 6.0 * frac**2 + 4.0) / 6.0,
        (-3.0 * frac**3 + 3.0 * frac**2 + 3.0 * frac + 1.0) / 6.0,
        frac**3 / 6.0,
    )
    matrix = np.zeros((count, columns))
    for tap in range(4):
        for v in range(count):
            column = cell[v] - 1 + tap + offset
            if 0 <= column < columns:
                matrix[v, column] += weights[tap][v]
    return matrix


def halves(x):
    x = np.asarray(x, np.float32)
    high = x.astype(jnp.bfloat16)
    low = (x - high.astype(np.float32)).astype(jnp.bfloat16)
    return high, low


def constants():
    bz = basis_matrix(CZ, A, 1)
    by = basis_matrix(CY, B, 1)
    bx = basis_matrix(NX, CE, 0)
    kron12 = np.einsum("za,yb->zyab", bz, by[:, :BP]).reshape(CZ * CY, ROWS)
    high, low = halves(kron12)
    pad = np.zeros((CZ * CY, 256 - 3 * ROWS), jnp.bfloat16)
    kd = np.concatenate([high, high, low, pad], axis=1)
    kron16 = np.einsum("za,yb->abzy", bz, by).reshape(A * B, CZ * CY)
    ke = np.concatenate(halves(kron16), axis=0)
    spread = np.zeros((LANES, 3 * NX))
    for c in range(3):
        spread[c * CE : (c + 1) * CE, c * NX : (c + 1) * NX] = bx.T
    high, low = halves(spread)
    bxd = np.concatenate([high, low], axis=0)
    bxe = np.concatenate([high.T, low.T], axis=1)
    dx = np.zeros((NX, NX))
    for step, weight in ((1, 45.0), (2, -9.0), (3, 1.0)):
        for v in range(NX):
            if v + step < NX:
                dx[v + step, v] = weight
            if v - step >= 0:
                dx[v - step, v] = -weight
    return kd, ke, bxd, bxe, dx.astype(jnp.bfloat16)


def split(x):
    high = x.astype(BF16)
    return high, (x - high.astype(F32)).astype(BF16)


def dot(a, b):
    return jnp.dot(a, b, preferred_element_type=F32)


def kernel(nz, ny, fixed, moving, kd_h, ke_h, bxd_h, bxe_h, dx_h, upd, res,
           fv, mv, mp, fl, ml, fh, mh, yls, yhs, zlr, zhr, ylr, yhr,
           g, u, cs, p3, tot, kd, ke, bxd, bxe, dx,
           enc, yst, rz, ry, rc, ars, arr,
           lsem, hss, hrs, xss, xrs, ass, arsem):
    d = lax.axis_index("gz")
    e = lax.axis_index("gy")
    up, down = lax.rem(d + 1, nz), lax.rem(d + nz - 1, nz)
    right, left = lax.rem(e + 1, ny), lax.rem(e + ny - 1, ny)

    barrier = pltpu.get_barrier_semaphore()

    def greet_y(k, carry):
        pl.semaphore_signal(barrier, inc=1, device_id=(d, lax.rem(e + k, ny)), device_id_type=MESH)
        return carry

    def greet_z(k, carry):
        pl.semaphore_signal(barrier, inc=1, device_id=(lax.rem(d + k, nz), e), device_id_type=MESH)
        return carry

    for z in (up, down):
        for y in (right, left):
            pl.semaphore_signal(barrier, inc=1, device_id=(z, y), device_id_type=MESH)
    lax.fori_loop(1, ny, greet_y, 0)
    lax.fori_loop(1, nz, greet_z, 0)

    def local(k, src, dst):
        copy = pltpu.make_async_copy(src, dst, lsem.at[k])
        copy.start()
        return copy

    faces_z = [
        local(0, fixed.at[pl.ds(0, 3)], fv.at[pl.ds(0, 3)]),
        local(1, moving.at[pl.ds(0, 3)], mv.at[pl.ds(0, 3)]),
        local(2, fixed.at[pl.ds(CZ - 3, 3)], fv.at[pl.ds(CZ - 3, 3)]),
        local(3, moving.at[pl.ds(CZ - 3, 3)], mv.at[pl.ds(CZ - 3, 3)]),
    ]
    faces_y = [
        local(4, fixed.at[:, pl.ds(0, 8)], fl),
        local(5, moving.at[:, pl.ds(0, 8)], ml),
        local(6, fixed.at[:, pl.ds(CY - 8, 8)], fh),
        local(7, moving.at[:, pl.ds(CY - 8, 8)], mh),
    ]
    rest = [
        local(8, fixed.at[pl.ds(3, CZ - 6)], fv.at[pl.ds(3, CZ - 6)]),
        local(9, moving.at[pl.ds(3, CZ - 6)], mv.at[pl.ds(3, CZ - 6)]),
        local(10, dx_h, dx),
        local(11, bxe_h, bxe),
    ]

    def remote(src, dst, send, recv, z, y):
        return pltpu.make_async_remote_copy(
            src_ref=src, dst_ref=dst, send_sem=send, recv_sem=recv, device_id=(z, y), device_id_type=MESH
        )

    for copy in faces_z:
        copy.wait()
    for z in (0, 1, 2, CZ - 3, CZ - 2, CZ - 1):
        mp[z + 3, 8 : 8 + CY, :] = 0.5 * (fv[z] + mv[z])
    for copy in faces_y:
        copy.wait()
    yls[...] = 0.5 * (fl[:, 0:4, :] + ml[:, 0:4, :])
    yhs[...] = 0.5 * (fh[:, 4:8, :] + mh[:, 4:8, :])
    pl.semaphore_wait(barrier, 4 + (ny - 1) + (nz - 1))
    halo = [
        remote(mp.at[pl.ds(CZ, 3), pl.ds(8, CY)], zlr, hss.at[0], hrs.at[0], up, e),
        remote(mp.at[pl.ds(3, 3), pl.ds(8, CY)], zhr, hss.at[1], hrs.at[1], down, e),
        remote(yhs, ylr, hss.at[2], hrs.at[2], d, right),
        remote(yls, yhr, hss.at[3], hrs.at[3], d, left),
    ]
    for copy in halo:
        copy.start()

    has_down = jnp.where(d > 0, 1.0, 0.0).astype(F32)
    has_up = jnp.where(d < nz - 1, 1.0, 0.0).astype(F32)
    has_left = jnp.where(e > 0, 1.0, 0.0).astype(F32)
    has_right = jnp.where(e < ny - 1, 1.0, 0.0).astype(F32)
    p3[...] = jnp.zeros_like(p3)

    for copy in rest:
        copy.wait()
    later = [local(12, ke_h, ke), local(13, bxd_h, bxd), local(14, kd_h, kd)]

    def fill(z, carry):
        mp[z + 3, 8 : 8 + CY, :] = 0.5 * (fv[z] + mv[z])
        return carry

    lax.fori_loop(3, CZ - 3, fill, 0)

    halo[2].wait_recv()
    mp[3 : CZ + 3, 4:8, :] = has_left * ylr[...]
    halo[3].wait_recv()
    mp[3 : CZ + 3, 8 + CY : 12 + CY, :] = has_right * yhr[...]

    def gather_x(volume, rows):
        total = None
        for c in range(3):
            term = dot(volume[c].astype(BF16), bxe[c * NX : (c + 1) * NX, :])
            total = term if total is None else total + term
        high, low = split(total[:, :LANES] + total[:, LANES:])
        u[rows, 0:LANES] = high
        u[rows, LANES : 2 * LANES] = low

    def first(z, layers):
        count = layers * CY
        rows = pl.ds(pl.multiple_of(z * CY, CY * OUTER), count)

        def along_z(k):
            return mp[pl.ds(z + 3 + k, layers), 8 : 8 + CY, :]

        def along_y(k):
            return mp[pl.ds(z + 3, layers), 8 + k : 8 + k + CY, :]

        def difference(part):
            return 45.0 * (part(1) - part(-1)) - 9.0 * (part(2) - part(-2)) + (part(3) - part(-3))

        high, low = split(along_z(0).reshape(count, NX))
        sixtieth = 1.0 / 60.0
        slopes = (
            difference(along_z).reshape(count, NX),
            difference(along_y).reshape(count, NX),
            dot(high, dx[...]) + dot(low, dx[...]),
        )
        mismatch = (fv[pl.ds(z, layers)] - mv[pl.ds(z, layers)]).reshape(count, NX)
        volume = []
        for c in range(3):
            rounded = (slopes[c] * sixtieth).astype(BF16)
            g[c, rows, :] = rounded
            volume.append(rounded.astype(F32) * mismatch)
        gather_x(volume, rows)

    def first_inner(t, carry):
        first(OUTER + t * INNER, INNER)
        return carry

    lax.fori_loop(0, (CZ - 2 * OUTER) // INNER, first_inner, 0)
    halo[0].wait_recv()
    mp[0:3, 8 : 8 + CY, :] = has_down * zlr[...]
    halo[1].wait_recv()
    mp[CZ + 3 : CZ + 6, 8 : 8 + CY, :] = has_up * zhr[...]

    def first_outer(t, carry):
        first(t * (CZ - OUTER), OUTER)
        return carry

    lax.fori_loop(0, 2, first_outer, 0)
    for copy in later:
        copy.wait()

    row = lax.broadcasted_iota(jnp.int32, (1, 4, LANES), 1)
    low_rows = jnp.where(row < 3, 1.0, 0.0).astype(F32)
    from_right = has_right * low_rows
    pa = lax.broadcasted_iota(jnp.int32, (A, B, LANES), 0) + (d * CA - 1)
    pb = lax.broadcasted_iota(jnp.int32, (A, B, LANES), 1) + (e * CB - 1)
    ia = lax.broadcasted_iota(jnp.int32, (A, B, LANES), 0)
    ib = lax.broadcasted_iota(jnp.int32, (A, B, LANES), 1)
    inside = (pa >= 0) & (pa < nz * CA) & (pb >= 0) & (pb < ny * CB) & (ib < 11)
    inside = jnp.where(inside, 1.0, 0.0).astype(F32)
    own = jnp.where((ia >= 1) & (ia < 1 + CA) & (ib >= 1) & (ib < 1 + CB), 1.0, 0.0).astype(F32)

    def exchange(k):
        both = dot(ke[...], u[...])
        half = A * B
        total = both[:half, :LANES] + both[half:, :LANES] + both[:half, LANES:]
        total = total.reshape(A, B, LANES)
        enc[k] = total
        yst[k, 0] = total[:, 8:12]
        yst[k, 1] = total[:, 0:4]
        src, after, before = enc.at[k], yst.at[k, 0], yst.at[k, 1]
        top, bottom = pl.ds(A - 3, 3), pl.ds(0, 3)
        copies = [
            remote(after.at[top], rc.at[k, 0], xss.at[k, 0], xrs.at[k, 0], up, right),
            remote(before.at[top], rc.at[k, 1], xss.at[k, 1], xrs.at[k, 1], up, left),
            remote(after.at[bottom], rc.at[k, 2], xss.at[k, 2], xrs.at[k, 2], down, right),
            remote(before.at[bottom], rc.at[k, 3], xss.at[k, 3], xrs.at[k, 3], down, left),
            remote(src.at[top], rz.at[k, 0], xss.at[k, 4], xrs.at[k, 4], up, e),
            remote(src.at[bottom], rz.at[k, 1], xss.at[k, 5], xrs.at[k, 5], down, e),
            remote(after, ry.at[k, 0], xss.at[k, 6], xrs.at[k, 6], d, right),
            remote(before, ry.at[k, 1], xss.at[k, 7], xrs.at[k, 7], d, left),
        ]
        for copy in copies:
            copy.start()
        return copies

    def collect(k, copies):
        for copy in copies:
            copy.wait_recv()
        tot[...] = enc[k]
        tot[0:3] += has_down * rz[k, 0]
        tot[4:7] += has_up * rz[k, 1]
        tot[:, 0:4] += has_left * ry[k, 0]
        tot[:, 8:12] += from_right * ry[k, 1]
        tot[0:3, 0:4] += (has_down * has_left) * rc[k, 0]
        tot[0:3, 8:12] += has_down * from_right * rc[k, 1]
        tot[4:7, 0:4] += (has_up * has_left) * rc[k, 2]
        tot[4:7, 8:12] += has_up * from_right * rc[k, 3]
        return tot[...] * inside

    def spread_x(control):
        for t in range(3):
            for a in range(A):
                p3[t * ROWS + a * BP : t * ROWS + (a + 1) * BP, :] = control[a, 0:BP, :]
        high, low = split(p3[...])
        wide = dot(jnp.concatenate([high, high], axis=1), bxd[...]) + dot(low, bxd[0:LANES, :])
        index = lax.broadcasted_iota(jnp.int32, (256, 3 * NX), 0)
        middle = (index >= ROWS) & (index < 2 * ROWS)
        rounded = wide.astype(BF16).astype(F32)
        cs[...] = jnp.where(middle, wide - rounded, rounded).astype(BF16)

    def apply(j, carry):
        rows = pl.ds(pl.multiple_of(j * CHUNK, CHUNK), CHUNK)
        field = dot(kd[rows, :], cs[...])
        slopes = [g[c, rows, :].astype(F32) for c in range(3)]
        s = slopes[0] * field[:, 0:NX]
        s = s + slopes[1] * field[:, NX : 2 * NX]
        s = s + slopes[2] * field[:, 2 * NX : 3 * NX]
        gather_x([slopes[c] * s for c in range(3)], rows)
        return carry + jnp.sum((s * s).reshape(CHUNK // 8, 8, NX), axis=0)

    def fold(x):
        total = jnp.sum(x, axis=0, keepdims=True)
        return total[:, 0:LANES] + total[:, LANES : 2 * LANES]

    def tile_sum(x):
        return jnp.sum(jnp.sum(x, axis=0), axis=0, keepdims=True)

    def reduce_start(stage, value):
        me, count = (e, ny) if stage == 0 else (d, nz)
        ars[stage] = value
        arr[stage, me] = value

        def send(k, carry):
            other = lax.rem(me + k, count)
            z, y = (d, other) if stage == 0 else (other, e)
            remote(ars.at[stage], arr.at[stage, me], ass.at[stage, k], arsem.at[stage, me], z, y).start()
            return carry

        lax.fori_loop(1, count, send, 0)

    def reduce_end(stage):
        me, count = (e, ny) if stage == 0 else (d, nz)

        def take(k, carry):
            other = lax.rem(me + count - k, count)
            remote(ars.at[stage], arr.at[stage, other], ass.at[stage, k], arsem.at[stage, other], d, e).wait_recv()
            return carry

        lax.fori_loop(1, count, take, 0)
        return jnp.sum(arr[stage], axis=0)

    zero = jnp.zeros((8, NX), F32)
    copies0 = exchange(0)
    r0 = collect(0, copies0)
    spread_x(r0)
    energy0 = fold(lax.fori_loop(0, STEPS, apply, zero))
    copies1 = exchange(1)
    t = collect(1, copies1)
    spread_x(t)
    energy1 = fold(lax.fori_loop(0, STEPS, apply, zero))
    sums = [tile_sum(r0 * r0 * own), energy0, tile_sum(t * t * own), energy1]
    reduce_start(0, jnp.concatenate(sums, axis=0))
    copies2 = exchange(2)
    reduce_start(1, reduce_end(0))
    t2 = collect(2, copies2)
    total = jnp.sum(reduce_end(1), axis=1, keepdims=True)
    rr0 = total[0:1]
    m1, m2, m3 = (total[k : k + 1] / rr0 for k in (1, 2, 3))
    alpha0 = 1.0 / (m1 + DAMPING)
    beta = alpha0 * alpha0 * (m2 - m1 * m1)
    curve = alpha0 * alpha0 * ((m3 - m1 * m2) - m1 * (m2 - m1 * m1)) + DAMPING * beta
    alpha1 = beta / (curve - beta * beta / alpha0)
    m1, alpha0, alpha1, beta = (x.reshape(1, 1, 1) for x in (m1, alpha0, alpha1, beta))
    r1 = alpha0 * (m1 * r0 - t)
    direction = r1 + beta * r0
    along = alpha0 * (m1 * t - t2) + DAMPING * r1 + beta * (t + DAMPING * r0)
    update = alpha0 * r0 + alpha1 * direction
    residual = r1 - alpha1 * along
    for c in range(3):
        upd[c] = update[1 : 1 + CA, 1 : 1 + CB, c * CE : (c + 1) * CE]
        res[c] = residual[1 : 1 + CA, 1 : 1 + CB, c * CE : (c + 1) * CE]

    for copy in halo + copies0 + copies1 + copies2:
        copy.wait_send()
    for stage in range(2):
        count = ny if stage == 0 else nz

        def sent(k, carry):
            remote(ars.at[stage], arr.at[stage, 0], ass.at[stage, k], arsem.at[stage, 0], d, e).wait_send()
            return carry

        lax.fori_loop(1, count, sent, 0)


def solution(mesh):
    nz, ny = mesh.shape["gz"], mesh.shape["gy"]
    tables = constants()
    count = max(nz, ny)
    vmem = pltpu.VMEM
    dma = pltpu.SemaphoreType.DMA
    scratch = [
        vmem((CZ, CY, NX), F32), vmem((CZ, CY, NX), F32),
        vmem((CZ + 6, CY + 16, NX), F32),
        vmem((CZ, 8, NX), F32), vmem((CZ, 8, NX), F32), vmem((CZ, 8, NX), F32), vmem((CZ, 8, NX), F32),
        vmem((CZ, 4, NX), F32), vmem((CZ, 4, NX), F32),
        vmem((3, CY, NX), F32), vmem((3, CY, NX), F32),
        vmem((CZ, 4, NX), F32), vmem((CZ, 4, NX), F32),
        vmem((3, CZ * CY, NX), BF16),
        vmem((CZ * CY, 2 * LANES), BF16),
        vmem((256, 3 * NX), BF16),
        vmem((256, LANES), F32),
        vmem((A, B, LANES), F32),
    ] + [vmem(t.shape, BF16) for t in tables] + [
        vmem((3, A, B, LANES), F32),
        vmem((3, 2, A, 4, LANES), F32),
        vmem((3, 2, 3, B, LANES), F32),
        vmem((3, 2, A, 4, LANES), F32),
        vmem((3, 4, 3, 4, LANES), F32),
        vmem((2, 4, LANES), F32),
        vmem((2, count, 4, LANES), F32),
        dma((15,)), dma((4,)), dma((4,)), dma((3, 8)), dma((3, 8)), dma((2, count)), dma((2, count)),
    ]
    out = jax.ShapeDtypeStruct((3, CA, CB, CE), F32)
    call = pl.pallas_call(
        functools.partial(kernel, nz, ny),
        out_shape=(out, out),
        in_specs=[pl.BlockSpec(memory_space=pl.ANY)] * 7,
        out_specs=(pl.BlockSpec(memory_space=pltpu.VMEM), pl.BlockSpec(memory_space=pltpu.VMEM)),
        scratch_shapes=scratch,
        compiler_params=pltpu.CompilerParams(collective_id=0, has_side_effects=True, vmem_limit_bytes=56 * 1024 * 1024),
        name="cg_step",
    )

    def shards(fixed, moving):
        return call(fixed, moving, *[jnp.asarray(t) for t in tables])

    return jax.shard_map(
        shards,
        mesh=mesh,
        in_specs=(P("gz", "gy", None), P("gz", "gy", None)),
        out_specs=(P(None, "gz", "gy", None), P(None, "gz", "gy", None)),
        check_vma=False,
    )
```

```python
import functools

import jax
import jax.numpy as jnp
import numpy as np
from jax import lax
from jax.experimental import pallas as pl
from jax.experimental.pallas import tpu as pltpu
from jax.sharding import PartitionSpec as P

SPACING = 8
DAMPING = 8.0
CZ, CY, NX = 32, 64, 256
CA, CB, CE = 4, 8, 32
A, B, LANES = 7, 16, 128
BP = 12
ROWS = A * BP
CHUNK = 2048
STEPS = CZ * CY // CHUNK
INNER = 8
OUTER = 4
MESH = pl.DeviceIdType.MESH
F32, BF16 = jnp.float32, jnp.bfloat16


def basis_matrix(count, columns, offset):
    voxel = np.arange(count)
    cell = voxel // SPACING
    frac = (voxel % SPACING + 0.5) / SPACING
    other = 1.0 - frac
    weights = (
        other**3 / 6.0,
        (3.0 * frac**3 - 6.0 * frac**2 + 4.0) / 6.0,
        (-3.0 * frac**3 + 3.0 * frac**2 + 3.0 * frac + 1.0) / 6.0,
        frac**3 / 6.0,
    )
    matrix = np.zeros((count, columns))
    for tap in range(4):
        for v in range(count):
            column = cell[v] - 1 + tap + offset
            if 0 <= column < columns:
                matrix[v, column] += weights[tap][v]
    return matrix


def halves(x):
    x = np.asarray(x, np.float32)
    high = x.astype(jnp.bfloat16)
    low = (x - high.astype(np.float32)).astype(jnp.bfloat16)
    return high, low


def constants():
    bz = basis_matrix(CZ, A, 1)
    by = basis_matrix(CY, B, 1)
    bx = basis_matrix(NX, CE, 0)
    kron12 = np.einsum("za,yb->zyab", bz, by[:, :BP]).reshape(CZ * CY, ROWS)
    high, low = halves(kron12)
    pad = np.zeros((CZ * CY, 256 - 3 * ROWS), jnp.bfloat16)
    kd = np.concatenate([high, high, low, pad], axis=1)
    kron16 = np.einsum("za,yb->abzy", bz, by).reshape(A * B, CZ * CY)
    ke = np.concatenate(halves(kron16), axis=0)
    spread = np.zeros((LANES, 3 * NX))
    for c in range(3):
        spread[c * CE : (c + 1) * CE, c * NX : (c + 1) * NX] = bx.T
    high, low = halves(spread)
    bxd = np.concatenate([high, low], axis=0)
    bxe = np.concatenate([high.T, low.T], axis=1)
    dx = np.zeros((NX, NX))
    for step, weight in ((1, 45.0), (2, -9.0), (3, 1.0)):
        for v in range(NX):
            if v + step < NX:
                dx[v + step, v] = weight
            if v - step >= 0:
                dx[v - step, v] = -weight
    return kd, ke, bxd, bxe, dx.astype(jnp.bfloat16)


def split(x):
    high = x.astype(BF16)
    return high, (x - high.astype(F32)).astype(BF16)


def dot(a, b):
    return jnp.dot(a, b, preferred_element_type=F32)


def kernel(nz, ny, fixed, moving, kd_h, ke_h, bxd_h, bxe_h, dx_h, out,
           fv, mv, mp, fl, ml, fh, mh, yls, yhs, zlr, zhr, ylr, yhr,
           g, along_s, u, cs, p3, tot, kd, ke, bxd, bxe, dx,
           enc, yst, rz, ry, rc, ars, arr,
           lsem, hss, hrs, xss, xrs, ass, arsem):
    d = lax.axis_index("gz")
    e = lax.axis_index("gy")
    up, down = lax.rem(d + 1, nz), lax.rem(d + nz - 1, nz)
    right, left = lax.rem(e + 1, ny), lax.rem(e + ny - 1, ny)

    has_down, has_up, has_left, has_right = d > 0, d < nz - 1, e > 0, e < ny - 1

    def clear(missing, refs):
        @pl.when(jnp.logical_not(missing))
        def _():
            for ref in refs:
                ref[...] = jnp.zeros(ref.shape, F32)

    barrier = pltpu.get_barrier_semaphore()

    def greet_y(k, carry):
        pl.semaphore_signal(barrier, inc=1, device_id=(d, lax.rem(e + k, ny)), device_id_type=MESH)
        return carry

    def greet_z(k, carry):
        pl.semaphore_signal(barrier, inc=1, device_id=(lax.rem(d + k, nz), e), device_id_type=MESH)
        return carry

    for z in (up, down):
        for y in (right, left):
            pl.semaphore_signal(barrier, inc=1, device_id=(z, y), device_id_type=MESH)
    lax.fori_loop(1, ny, greet_y, 0)
    lax.fori_loop(1, nz, greet_z, 0)

    clear(has_down, [zlr] + [rz.at[k, 0] for k in range(3)])
    clear(has_up, [zhr] + [rz.at[k, 1] for k in range(3)])
    clear(has_left, [ylr] + [ry.at[k, 0] for k in range(3)])
    clear(has_right, [yhr] + [ry.at[k, 1] for k in range(3)])
    clear(has_down & has_left, [rc.at[k, 0] for k in range(3)])
    clear(has_down & has_right, [rc.at[k, 1] for k in range(3)])
    clear(has_up & has_left, [rc.at[k, 2] for k in range(3)])
    clear(has_up & has_right, [rc.at[k, 3] for k in range(3)])

    def local(k, src, dst):
        copy = pltpu.make_async_copy(src, dst, lsem.at[k])
        copy.start()
        return copy

    faces_z = [
        local(0, fixed.at[pl.ds(0, 3)], fv.at[pl.ds(0, 3)]),
        local(1, moving.at[pl.ds(0, 3)], mv.at[pl.ds(0, 3)]),
        local(2, fixed.at[pl.ds(CZ - 3, 3)], fv.at[pl.ds(CZ - 3, 3)]),
        local(3, moving.at[pl.ds(CZ - 3, 3)], mv.at[pl.ds(CZ - 3, 3)]),
    ]
    faces_y = [
        local(4, fixed.at[:, pl.ds(0, 8)], fl),
        local(5, moving.at[:, pl.ds(0, 8)], ml),
        local(6, fixed.at[:, pl.ds(CY - 8, 8)], fh),
        local(7, moving.at[:, pl.ds(CY - 8, 8)], mh),
    ]
    rest = [
        local(8, fixed.at[pl.ds(3, CZ - 6)], fv.at[pl.ds(3, CZ - 6)]),
        local(9, moving.at[pl.ds(3, CZ - 6)], mv.at[pl.ds(3, CZ - 6)]),
        local(10, dx_h, dx),
        local(11, bxe_h, bxe),
    ]

    def remote(src, dst, send, recv, z, y):
        return pltpu.make_async_remote_copy(
            src_ref=src, dst_ref=dst, send_sem=send, recv_sem=recv, device_id=(z, y), device_id_type=MESH
        )

    for copy in faces_z:
        copy.wait()
    for z in (0, 1, 2, CZ - 3, CZ - 2, CZ - 1):
        mp[z + 3, 8 : 8 + CY, :] = 0.5 * (fv[z] + mv[z])
    pl.semaphore_wait(barrier, 4 + (ny - 1) + (nz - 1))
    halo = [
        remote(mp.at[pl.ds(CZ, 3), pl.ds(8, CY)], zlr, hss.at[0], hrs.at[0], up, e),
        remote(mp.at[pl.ds(3, 3), pl.ds(8, CY)], zhr, hss.at[1], hrs.at[1], down, e),
        remote(yhs, ylr, hss.at[2], hrs.at[2], d, right),
        remote(yls, yhr, hss.at[3], hrs.at[3], d, left),
    ]
    pl.when(has_up)(halo[0].start)
    pl.when(has_down)(halo[1].start)
    for copy in faces_y:
        copy.wait()
    yls[...] = 0.5 * (fl[:, 0:4, :] + ml[:, 0:4, :])
    yhs[...] = 0.5 * (fh[:, 4:8, :] + mh[:, 4:8, :])
    pl.when(has_right)(halo[2].start)
    pl.when(has_left)(halo[3].start)
    p3[...] = jnp.zeros_like(p3)

    for copy in rest:
        copy.wait()
    later = [local(12, ke_h, ke), local(13, bxd_h, bxd), local(14, kd_h, kd)]

    def fill(z, carry):
        mp[z + 3, 8 : 8 + CY, :] = 0.5 * (fv[z] + mv[z])
        return carry

    lax.fori_loop(3, CZ - 3, fill, 0)

    pl.when(has_left)(halo[2].wait_recv)
    mp[3 : CZ + 3, 4:8, :] = ylr[...]
    pl.when(has_right)(halo[3].wait_recv)
    mp[3 : CZ + 3, 8 + CY : 12 + CY, :] = yhr[...]

    def gather_x(volume, rows):
        total = None
        for c in range(3):
            term = dot(volume[c].astype(BF16), bxe[c * NX : (c + 1) * NX, :])
            total = term if total is None else total + term
        high, low = split(total[:, :LANES] + total[:, LANES:])
        u[rows, 0:LANES] = high
        u[rows, LANES : 2 * LANES] = low

    def first(z, layers):
        count = layers * CY
        rows = pl.ds(pl.multiple_of(z * CY, CY * OUTER), count)

        def along_z(k):
            return mp[pl.ds(z + 3 + k, layers), 8 : 8 + CY, :]

        def along_y(k):
            return mp[pl.ds(z + 3, layers), 8 + k : 8 + k + CY, :]

        def difference(part):
            return 45.0 * (part(1) - part(-1)) - 9.0 * (part(2) - part(-2)) + (part(3) - part(-3))

        high, low = split(along_z(0).reshape(count, NX))
        sixtieth = 1.0 / 60.0
        slopes = (
            difference(along_z).reshape(count, NX),
            difference(along_y).reshape(count, NX),
            dot(high, dx[...]) + dot(low, dx[...]),
        )
        mismatch = (fv[pl.ds(z, layers)] - mv[pl.ds(z, layers)]).reshape(count, NX)
        volume = []
        for c in range(3):
            rounded = (slopes[c] * sixtieth).astype(BF16)
            g[c, rows, :] = rounded
            volume.append(rounded.astype(F32) * mismatch)
        gather_x(volume, rows)

    def first_inner(t, carry):
        first(OUTER + t * INNER, INNER)
        return carry

    lax.fori_loop(0, (CZ - 2 * OUTER) // INNER, first_inner, 0)
    pl.when(has_down)(halo[0].wait_recv)
    mp[0:3, 8 : 8 + CY, :] = zlr[...]
    pl.when(has_up)(halo[1].wait_recv)
    mp[CZ + 3 : CZ + 6, 8 : 8 + CY, :] = zhr[...]

    def first_outer(t, carry):
        first(t * (CZ - OUTER), OUTER)
        return carry

    lax.fori_loop(0, 2, first_outer, 0)
    for copy in later:
        copy.wait()

    row = lax.broadcasted_iota(jnp.int32, (1, 4, LANES), 1)
    low_rows = jnp.where(row < 3, 1.0, 0.0).astype(F32)
    pa = lax.broadcasted_iota(jnp.int32, (A, B, LANES), 0) + (d * CA - 1)
    pb = lax.broadcasted_iota(jnp.int32, (A, B, LANES), 1) + (e * CB - 1)
    ia = lax.broadcasted_iota(jnp.int32, (A, B, LANES), 0)
    ib = lax.broadcasted_iota(jnp.int32, (A, B, LANES), 1)
    inside = (pa >= 0) & (pa < nz * CA) & (pb >= 0) & (pb < ny * CB) & (ib < 11)
    inside = jnp.where(inside, 1.0, 0.0).astype(F32)
    own = jnp.where((ia >= 1) & (ia < 1 + CA) & (ib >= 1) & (ib < 1 + CB), 1.0, 0.0).astype(F32)

    targets = (has_up & has_right, has_up & has_left, has_down & has_right, has_down & has_left,
               has_up, has_down, has_right, has_left)
    sources = (has_down & has_left, has_down & has_right, has_up & has_left, has_up & has_right,
               has_down, has_up, has_left, has_right)

    def exchange(k):
        both = dot(ke[...], u[...])
        half = A * B
        total = both[:half, :LANES] + both[half:, :LANES] + both[:half, LANES:]
        total = total.reshape(A, B, LANES)
        enc[k] = total
        yst[k, 0] = total[:, 8:12]
        yst[k, 1] = total[:, 0:4]
        src, after, before = enc.at[k], yst.at[k, 0], yst.at[k, 1]
        top, bottom = pl.ds(A - 3, 3), pl.ds(0, 3)
        copies = [
            remote(after.at[top], rc.at[k, 0], xss.at[k, 0], xrs.at[k, 0], up, right),
            remote(before.at[top], rc.at[k, 1], xss.at[k, 1], xrs.at[k, 1], up, left),
            remote(after.at[bottom], rc.at[k, 2], xss.at[k, 2], xrs.at[k, 2], down, right),
            remote(before.at[bottom], rc.at[k, 3], xss.at[k, 3], xrs.at[k, 3], down, left),
            remote(src.at[top], rz.at[k, 0], xss.at[k, 4], xrs.at[k, 4], up, e),
            remote(src.at[bottom], rz.at[k, 1], xss.at[k, 5], xrs.at[k, 5], down, e),
            remote(after, ry.at[k, 0], xss.at[k, 6], xrs.at[k, 6], d, right),
            remote(before, ry.at[k, 1], xss.at[k, 7], xrs.at[k, 7], d, left),
        ]
        for copy, target in zip(copies, targets):
            pl.when(target)(copy.start)
        return copies

    def collect(k, copies):
        for copy, source in zip(copies, sources):
            pl.when(source)(copy.wait_recv)
        tot[...] = enc[k]
        tot[0:3] += rz[k, 0]
        tot[4:7] += rz[k, 1]
        tot[:, 0:4] += ry[k, 0]
        tot[:, 8:12] += low_rows * ry[k, 1]
        tot[0:3, 0:4] += rc[k, 0]
        tot[0:3, 8:12] += low_rows * rc[k, 1]
        tot[4:7, 0:4] += rc[k, 2]
        tot[4:7, 8:12] += low_rows * rc[k, 3]
        return tot[...] * inside

    def spread_x(control):
        for t in range(3):
            for a in range(A):
                p3[t * ROWS + a * BP : t * ROWS + (a + 1) * BP, :] = control[a, 0:BP, :]
        high, low = split(p3[...])
        wide = dot(jnp.concatenate([high, high], axis=1), bxd[...]) + dot(low, bxd[0:LANES, :])
        index = lax.broadcasted_iota(jnp.int32, (256, 3 * NX), 0)
        middle = (index >= ROWS) & (index < 2 * ROWS)
        rounded = wide.astype(BF16).astype(F32)
        cs[...] = jnp.where(middle, wide - rounded, rounded).astype(BF16)

    def through(rows):
        field = dot(kd[rows, :], cs[...])
        slopes = [g[c, rows, :].astype(F32) for c in range(3)]
        s = slopes[0] * field[:, 0:NX]
        s = s + slopes[1] * field[:, NX : 2 * NX]
        s = s + slopes[2] * field[:, 2 * NX : 3 * NX]
        return slopes, s

    def add_square(carry, s):
        return carry + jnp.sum((s * s).reshape(CHUNK // 8, 8, NX), axis=0)

    def step(j):
        return pl.ds(pl.multiple_of(j * CHUNK, CHUNK), CHUNK)

    def apply(j, carry):
        slopes, s = through(step(j))
        gather_x([slopes[c] * s for c in range(3)], step(j))
        return add_square(carry, s)

    def apply_forward(j, carry):
        unused, s = through(step(j))
        along_s[step(j), :] = s
        return add_square(carry, s)

    def apply_back(j, carry):
        s = along_s[step(j), :]
        gather_x([g[c, step(j), :].astype(F32) * s for c in range(3)], step(j))
        return carry

    def fold(x):
        total = jnp.sum(x, axis=0, keepdims=True)
        return total[:, 0:LANES] + total[:, LANES : 2 * LANES]

    def tile_sum(x):
        return jnp.sum(jnp.sum(x, axis=0), axis=0, keepdims=True)

    def reduce_start(stage, value):
        me, count = (e, ny) if stage == 0 else (d, nz)
        ars[stage] = value
        arr[stage, me] = value

        for k in sorted(range(1, count), key=lambda k: -min(k, count - k)):
            other = lax.rem(me + k, count)
            z, y = (d, other) if stage == 0 else (other, e)
            remote(ars.at[stage], arr.at[stage, me], ass.at[stage], arsem.at[stage], z, y).start()

    def reduce_end(stage):
        count = ny if stage == 0 else nz
        others = arr.at[stage, pl.ds(0, count - 1)]
        pltpu.make_async_copy(others, others, arsem.at[stage]).wait()
        return jnp.sum(arr[stage, 0:count], axis=0)

    zero = jnp.zeros((8, NX), F32)
    copies0 = exchange(0)
    r0 = collect(0, copies0)
    spread_x(r0)
    energy0 = fold(lax.fori_loop(0, STEPS, apply, zero))
    copies1 = exchange(1)
    t = collect(1, copies1)
    spread_x(t)
    energy1 = fold(lax.fori_loop(0, STEPS, apply_forward, zero))
    sums = [tile_sum(r0 * r0 * own), energy0, tile_sum(t * t * own), energy1]
    reduce_start(0, jnp.concatenate(sums, axis=0))
    lax.fori_loop(0, STEPS, apply_back, 0)
    copies2 = exchange(2)
    reduce_start(1, reduce_end(0))
    t2 = collect(2, copies2)
    total = jnp.sum(reduce_end(1), axis=1, keepdims=True)
    rr0 = total[0:1]
    m1, m2, m3 = (total[k : k + 1] / rr0 for k in (1, 2, 3))
    alpha0 = 1.0 / (m1 + DAMPING)
    beta = alpha0 * alpha0 * (m2 - m1 * m1)
    curve = alpha0 * alpha0 * ((m3 - m1 * m2) - m1 * (m2 - m1 * m1)) + DAMPING * beta
    alpha1 = beta / (curve - beta * beta / alpha0)
    m1, alpha0, alpha1, beta = (x.reshape(1, 1, 1) for x in (m1, alpha0, alpha1, beta))
    r1 = alpha0 * (m1 * r0 - t)
    direction = r1 + beta * r0
    along = alpha0 * (m1 * t - t2) + DAMPING * r1 + beta * (t + DAMPING * r0)
    parts = (alpha0 * r0, alpha1 * direction, r1, -alpha1 * along)
    for k, part in enumerate(parts):
        for c in range(3):
            out[k, c] = part[1 : 1 + CA, 1 : 1 + CB, c * CE : (c + 1) * CE]

    for copy, target in zip(halo + copies0 + copies1 + copies2, (has_up, has_down, has_right, has_left) + targets * 3):
        pl.when(target)(copy.wait_send)
    for stage in range(2):
        others = arr.at[stage, pl.ds(0, (ny if stage == 0 else nz) - 1)]
        pltpu.make_async_copy(others, others, ass.at[stage]).wait()


def solution(mesh):
    nz, ny = mesh.shape["gz"], mesh.shape["gy"]
    tables = constants()
    count = max(nz, ny)
    vmem = pltpu.VMEM
    dma = pltpu.SemaphoreType.DMA
    scratch = [
        vmem((CZ, CY, NX), F32), vmem((CZ, CY, NX), F32),
        vmem((CZ + 6, CY + 16, NX), F32),
        vmem((CZ, 8, NX), F32), vmem((CZ, 8, NX), F32), vmem((CZ, 8, NX), F32), vmem((CZ, 8, NX), F32),
        vmem((CZ, 4, NX), F32), vmem((CZ, 4, NX), F32),
        vmem((3, CY, NX), F32), vmem((3, CY, NX), F32),
        vmem((CZ, 4, NX), F32), vmem((CZ, 4, NX), F32),
        vmem((3, CZ * CY, NX), BF16),
        vmem((CZ * CY, NX), F32),
        vmem((CZ * CY, 2 * LANES), BF16),
        vmem((256, 3 * NX), BF16),
        vmem((256, LANES), F32),
        vmem((A, B, LANES), F32),
    ] + [vmem(t.shape, BF16) for t in tables] + [
        vmem((3, A, B, LANES), F32),
        vmem((3, 2, A, 4, LANES), F32),
        vmem((3, 2, 3, B, LANES), F32),
        vmem((3, 2, A, 4, LANES), F32),
        vmem((3, 4, 3, 4, LANES), F32),
        vmem((2, 4, LANES), F32),
        vmem((2, count, 4, LANES), F32),
        dma((15,)), dma((4,)), dma((4,)), dma((3, 8)), dma((3, 8)), dma((2,)), dma((2,)),
    ]
    out = jax.ShapeDtypeStruct((4, 3, CA, CB, CE), F32)
    call = pl.pallas_call(
        functools.partial(kernel, nz, ny),
        out_shape=out,
        in_specs=[pl.BlockSpec(memory_space=pl.ANY)] * 7,
        out_specs=pl.BlockSpec(memory_space=pltpu.VMEM),
        scratch_shapes=scratch,
        compiler_params=pltpu.CompilerParams(collective_id=0, has_side_effects=True, vmem_limit_bytes=56 * 1024 * 1024),
        name="cg_step",
    )

    def shards(fixed, moving):
        parts = call(fixed, moving, *[jnp.asarray(t) for t in tables])
        return parts[0] + parts[1], parts[2] + parts[3]

    return jax.shard_map(
        shards,
        mesh=mesh,
        in_specs=(P("gz", "gy", None), P("gz", "gy", None)),
        out_specs=(P(None, "gz", "gy", None), P(None, "gz", "gy", None)),
        check_vma=False,
    )
```

```python
import functools

import jax
import jax.numpy as jnp
import numpy as np
from jax import lax
from jax.experimental import pallas as pl
from jax.experimental.pallas import tpu as pltpu
from jax.sharding import PartitionSpec as P

SPACING = 8
DAMPING = 8.0
CZ, CY, NX = 32, 64, 256
CA, CB, CE = 4, 8, 32
A, B, LANES = 7, 16, 128
BP = 12
ROWS = A * BP
CHUNK = CZ * CY
INNER = 8
OUTER = 4
STRIPS = CZ * CY // NX
AT_BXE = NX
AT_BXD = AT_BXE + 3 * NX
AT_KE = AT_BXD + 6 * LANES
AT_KD = AT_KE + 2 * A * B * STRIPS
TABLE = AT_KD + CZ * CY
VMEM_BYTES = 63 * 1024 * 1024
MESH = pl.DeviceIdType.MESH
F32, BF16 = jnp.float32, jnp.bfloat16


def basis_matrix(count, columns, offset):
    voxel = np.arange(count)
    cell = voxel // SPACING
    frac = (voxel % SPACING + 0.5) / SPACING
    other = 1.0 - frac
    weights = (
        other**3 / 6.0,
        (3.0 * frac**3 - 6.0 * frac**2 + 4.0) / 6.0,
        (-3.0 * frac**3 + 3.0 * frac**2 + 3.0 * frac + 1.0) / 6.0,
        frac**3 / 6.0,
    )
    matrix = np.zeros((count, columns))
    for tap in range(4):
        for v in range(count):
            column = cell[v] - 1 + tap + offset
            if 0 <= column < columns:
                matrix[v, column] += weights[tap][v]
    return matrix


def halves(x):
    x = np.asarray(x, np.float32)
    high = x.astype(jnp.bfloat16)
    low = (x - high.astype(np.float32)).astype(jnp.bfloat16)
    return high, low


def constants():
    bz = basis_matrix(CZ, A, 1)
    by = basis_matrix(CY, B, 1)
    bx = basis_matrix(NX, CE, 0)
    kron12 = np.einsum("za,yb->zyab", bz, by[:, :BP]).reshape(CZ * CY, ROWS)
    high, low = halves(kron12)
    pad = np.zeros((CZ * CY, 256 - 3 * ROWS), jnp.bfloat16)
    kd = np.concatenate([high, high, low, pad], axis=1)
    kron16 = np.einsum("za,yb->abzy", bz, by).reshape(A * B, CZ * CY)
    ke = np.concatenate(halves(kron16), axis=0)
    spread = np.zeros((LANES, 3 * NX))
    for c in range(3):
        spread[c * CE : (c + 1) * CE, c * NX : (c + 1) * NX] = bx.T
    high, low = halves(spread)
    bxd = np.concatenate([high, low], axis=0)
    bxe = np.concatenate([high.T, low.T], axis=1)
    dx = np.zeros((NX, NX))
    for step, weight in ((1, 45.0), (2, -9.0), (3, 1.0)):
        for v in range(NX):
            if v + step < NX:
                dx[v + step, v] = weight
            if v - step >= 0:
                dx[v - step, v] = -weight
    bxd = bxd.reshape(2 * LANES, 3, NX).transpose(1, 0, 2).reshape(6 * LANES, NX)
    ke = ke.reshape(2 * A * B, STRIPS, NX).transpose(1, 0, 2).reshape(2 * A * B * STRIPS, NX)
    return np.concatenate([dx.astype(jnp.bfloat16), bxe, bxd, ke, kd], axis=0)


def split(x):
    high = x.astype(BF16)
    return high, (x - high.astype(F32)).astype(BF16)


def dot(a, b):
    return jnp.dot(a, b, preferred_element_type=F32)


def kernel(nz, ny, fixed, moving, tab_h, out,
           fv, mv, mp, fl, ml, fh, mh, yls, yhs, zlr, zhr, ylr, yhr,
           g, along_s, u, cs, p3, tot, up_x, tab,
           enc, yst, rz, ry, rc, ars, arr,
           lsem, hss, hrs, xss, xrs, ass, arsem):
    d = lax.axis_index("gz")
    e = lax.axis_index("gy")
    up, down = lax.rem(d + 1, nz), lax.rem(d + nz - 1, nz)
    right, left = lax.rem(e + 1, ny), lax.rem(e + ny - 1, ny)

    has_down, has_up, has_left, has_right = d > 0, d < nz - 1, e > 0, e < ny - 1

    def local(k, src, dst):
        copy = pltpu.make_async_copy(src, dst, lsem.at[k])
        copy.start()
        return copy

    faces_z = [
        local(0, fixed.at[pl.ds(0, 3)], fv.at[pl.ds(0, 3)]),
        local(1, moving.at[pl.ds(0, 3)], mv.at[pl.ds(0, 3)]),
        local(2, fixed.at[pl.ds(CZ - 3, 3)], fv.at[pl.ds(CZ - 3, 3)]),
        local(3, moving.at[pl.ds(CZ - 3, 3)], mv.at[pl.ds(CZ - 3, 3)]),
    ]
    faces_y = [
        local(4, fixed.at[:, pl.ds(0, 8)], fl),
        local(5, moving.at[:, pl.ds(0, 8)], ml),
        local(6, fixed.at[:, pl.ds(CY - 8, 8)], fh),
        local(7, moving.at[:, pl.ds(CY - 8, 8)], mh),
    ]
    rest = [
        local(8, fixed.at[pl.ds(3, CZ - 6)], fv.at[pl.ds(3, CZ - 6)]),
        local(9, moving.at[pl.ds(3, CZ - 6)], mv.at[pl.ds(3, CZ - 6)]),
        local(10, tab_h.at[pl.ds(0, 4 * NX)], tab.at[pl.ds(0, 4 * NX)]),
    ]

    barrier = pltpu.get_barrier_semaphore()

    def greet_y(k, carry):
        pl.semaphore_signal(barrier, inc=1, device_id=(d, lax.rem(e + k, ny)), device_id_type=MESH)
        return carry

    def greet_z(k, carry):
        pl.semaphore_signal(barrier, inc=1, device_id=(lax.rem(d + k, nz), e), device_id_type=MESH)
        return carry

    for z in (up, down):
        for y in (right, left):
            pl.semaphore_signal(barrier, inc=1, device_id=(z, y), device_id_type=MESH)
    lax.fori_loop(1, ny, greet_y, 0)
    lax.fori_loop(1, nz, greet_z, 0)

    def clear(missing, refs):
        @pl.when(jnp.logical_not(missing))
        def _():
            for ref in refs:
                ref[...] = jnp.zeros(ref.shape, F32)

    clear(has_down, [zlr] + [rz.at[k, 0] for k in range(3)])
    clear(has_up, [zhr] + [rz.at[k, 1] for k in range(3)])
    clear(has_left, [ylr] + [ry.at[k, 0] for k in range(3)])
    clear(has_right, [yhr] + [ry.at[k, 1] for k in range(3)])
    clear(has_down & has_left, [rc.at[k, 0] for k in range(3)])
    clear(has_down & has_right, [rc.at[k, 1] for k in range(3)])
    clear(has_up & has_left, [rc.at[k, 2] for k in range(3)])
    clear(has_up & has_right, [rc.at[k, 3] for k in range(3)])

    def remote(src, dst, send, recv, z, y):
        return pltpu.make_async_remote_copy(
            src_ref=src, dst_ref=dst, send_sem=send, recv_sem=recv, device_id=(z, y), device_id_type=MESH
        )

    for copy in faces_z:
        copy.wait()
    for z in (0, 1, 2, CZ - 3, CZ - 2, CZ - 1):
        mp[z + 3, 8 : 8 + CY, :] = 0.5 * (fv[z] + mv[z])
    pl.semaphore_wait(barrier, 4 + (ny - 1) + (nz - 1))
    halo = [
        remote(mp.at[pl.ds(CZ, 3), pl.ds(8, CY)], zlr, hss.at[0], hrs.at[0], up, e),
        remote(mp.at[pl.ds(3, 3), pl.ds(8, CY)], zhr, hss.at[1], hrs.at[1], down, e),
        remote(yhs, ylr, hss.at[2], hrs.at[2], d, right),
        remote(yls, yhr, hss.at[3], hrs.at[3], d, left),
    ]
    pl.when(has_up)(halo[0].start)
    pl.when(has_down)(halo[1].start)
    for copy in faces_y:
        copy.wait()
    yls[...] = 0.5 * (fl[:, 0:4, :] + ml[:, 0:4, :])
    yhs[...] = 0.5 * (fh[:, 4:8, :] + mh[:, 4:8, :])
    pl.when(has_right)(halo[2].start)
    pl.when(has_left)(halo[3].start)
    p3[...] = jnp.zeros_like(p3)

    for copy in rest:
        copy.wait()
    tail = pl.ds(4 * NX, TABLE - 4 * NX)
    later = [local(11, tab_h.at[tail], tab.at[tail])]

    def fill(z, carry):
        mp[z + 3, 8 : 8 + CY, :] = 0.5 * (fv[z] + mv[z])
        return carry

    lax.fori_loop(3, CZ - 3, fill, 0)

    def gather_x(volume):
        total = None
        for c in range(3):
            if volume[c] is None:
                continue
            term = dot(volume[c].astype(BF16), tab[AT_BXE + c * NX : AT_BXE + (c + 1) * NX, :])
            total = term if total is None else total + term
        return total[:, :LANES] + total[:, LANES:]

    def keep(total):
        high, low = split(total)
        u[...] = jnp.concatenate([high, low], axis=1).reshape(CZ, CY, 2 * LANES)

    edges, middle, every = ((0, 16), (CY - 16, 16)), ((16, CY - 32),), ((0, CY),)

    def first(z, layers, spans, parts, begun, done):
        count = layers * sum(size for unused, size in spans)
        deep = pl.ds(z, layers)

        def block(ref, dz, dy):
            pieces = [ref[pl.ds(z + dz, layers), dy + y : dy + y + size, :] for y, size in spans]
            whole = pieces[0] if len(pieces) == 1 else jnp.concatenate(pieces, axis=1)
            return whole.reshape(count, whole.shape[-1])

        def put(ref, value):
            value = value.reshape(layers, -1, value.shape[-1])
            at = 0
            for y, size in spans:
                ref[deep, y : y + size, :] = value[:, at : at + size]
                at += size

        def difference(part):
            return 45.0 * (part(1) - part(-1)) - 9.0 * (part(2) - part(-2)) + (part(3) - part(-3))

        mismatch = block(fv, 0, 0) - block(mv, 0, 0)
        volume = [None] * 3
        for c in parts:
            if c == 0:
                slope = difference(lambda k: block(mp, 3 + k, 8))
            elif c == 1:
                slope = difference(lambda k: block(mp, 3, 8 + k))
            else:
                high, low = split(block(mp, 3, 8))
                slope = dot(high, tab[0:NX, :]) + dot(low, tab[0:NX, :])
            rounded = (slope * (1.0 / 60.0)).astype(BF16)
            put(g.at[c], rounded)
            volume[c] = rounded.astype(F32) * mismatch
        total = gather_x(volume)
        if begun:
            total = total + block(up_x, 0, 0)
        if not done:
            put(up_x, total)
        else:
            high, low = split(total)
            put(u, jnp.concatenate([high, low], axis=1))

    inner, faces = (CZ - 2 * OUTER) // INNER, CZ - OUTER

    def own_inner(t, carry):
        first(OUTER + t * INNER, INNER, middle, (0, 1, 2), False, True)
        first(OUTER + t * INNER, INNER, edges, (0, 2), False, False)
        return carry

    def own_outer(t, carry):
        first(t * faces, OUTER, every, (2,), False, False)
        return carry

    def side_inner(t, carry):
        first(OUTER + t * INNER, INNER, edges, (1,), True, True)
        return carry

    def side_outer(t, carry):
        first(t * faces, OUTER, every, (1,), True, False)
        return carry

    def top_outer(t, carry):
        first(t * faces, OUTER, every, (0,), True, True)
        return carry

    lax.fori_loop(0, inner, own_inner, 0)
    lax.fori_loop(0, 2, own_outer, 0)
    pl.when(has_left)(halo[2].wait_recv)
    mp[3 : CZ + 3, 4:8, :] = ylr[...]
    pl.when(has_right)(halo[3].wait_recv)
    mp[3 : CZ + 3, 8 + CY : 12 + CY, :] = yhr[...]

    lax.fori_loop(0, inner, side_inner, 0)
    lax.fori_loop(0, 2, side_outer, 0)
    pl.when(has_down)(halo[0].wait_recv)
    mp[0:3, 8 : 8 + CY, :] = zlr[...]
    pl.when(has_up)(halo[1].wait_recv)
    mp[CZ + 3 : CZ + 6, 8 : 8 + CY, :] = zhr[...]
    lax.fori_loop(0, 2, top_outer, 0)
    for copy in later:
        copy.wait()

    row = lax.broadcasted_iota(jnp.int32, (1, 4, LANES), 1)
    low_rows = jnp.where(row < 3, 1.0, 0.0).astype(F32)
    pa = lax.broadcasted_iota(jnp.int32, (A, B, LANES), 0) + (d * CA - 1)
    pb = lax.broadcasted_iota(jnp.int32, (A, B, LANES), 1) + (e * CB - 1)
    ia = lax.broadcasted_iota(jnp.int32, (A, B, LANES), 0)
    ib = lax.broadcasted_iota(jnp.int32, (A, B, LANES), 1)
    inside = (pa >= 0) & (pa < nz * CA) & (pb >= 0) & (pb < ny * CB) & (ib < 11)
    inside = jnp.where(inside, 1.0, 0.0).astype(F32)
    own = jnp.where((ia >= 1) & (ia < 1 + CA) & (ib >= 1) & (ib < 1 + CB), 1.0, 0.0).astype(F32)

    targets = (has_up & has_right, has_up & has_left, has_down & has_right, has_down & has_left,
               has_up, has_down, has_right, has_left)
    sources = (has_down & has_left, has_down & has_right, has_up & has_left, has_up & has_right,
               has_down, has_up, has_left, has_right)

    def exchange(k):
        half = A * B
        both = None
        for n in range(STRIPS):
            strip = tab[AT_KE + n * 2 * half : AT_KE + (n + 1) * 2 * half, :]
            layers = NX // CY
            term = dot(strip, u[n * layers : (n + 1) * layers].reshape(NX, 2 * LANES))
            both = term if both is None else both + term
        total = both[:half, :LANES] + both[half:, :LANES] + both[:half, LANES:]
        total = total.reshape(A, B, LANES)
        enc[k] = total
        yst[k, 0] = total[:, 8:12]
        yst[k, 1] = total[:, 0:4]
        src, after, before = enc.at[k], yst.at[k, 0], yst.at[k, 1]
        top, bottom = pl.ds(A - 3, 3), pl.ds(0, 3)
        copies = [
            remote(after.at[top], rc.at[k, 0], xss.at[k, 0], xrs.at[k, 0], up, right),
            remote(before.at[top], rc.at[k, 1], xss.at[k, 1], xrs.at[k, 1], up, left),
            remote(after.at[bottom], rc.at[k, 2], xss.at[k, 2], xrs.at[k, 2], down, right),
            remote(before.at[bottom], rc.at[k, 3], xss.at[k, 3], xrs.at[k, 3], down, left),
            remote(src.at[top], rz.at[k, 0], xss.at[k, 4], xrs.at[k, 4], up, e),
            remote(src.at[bottom], rz.at[k, 1], xss.at[k, 5], xrs.at[k, 5], down, e),
            remote(after, ry.at[k, 0], xss.at[k, 6], xrs.at[k, 6], d, right),
            remote(before, ry.at[k, 1], xss.at[k, 7], xrs.at[k, 7], d, left),
        ]
        for copy, target in zip(copies, targets):
            pl.when(target)(copy.start)
        return copies

    def collect(k, copies):
        for copy, source in zip(copies, sources):
            pl.when(source)(copy.wait_recv)
        tot[...] = enc[k]
        tot[0:3] += rz[k, 0]
        tot[4:7] += rz[k, 1]
        tot[:, 0:4] += ry[k, 0]
        tot[:, 8:12] += low_rows * ry[k, 1]
        tot[0:3, 0:4] += rc[k, 0]
        tot[0:3, 8:12] += low_rows * rc[k, 1]
        tot[4:7, 0:4] += rc[k, 2]
        tot[4:7, 8:12] += low_rows * rc[k, 3]
        return tot[...] * inside

    def spread_x(control):
        for t in range(3):
            for a in range(A):
                p3[t * ROWS + a * BP : t * ROWS + (a + 1) * BP, :] = control[a, 0:BP, :]
        high, low = split(p3[...])
        twice = jnp.concatenate([high, high], axis=1)
        wide = []
        for c in range(3):
            at = AT_BXD + c * 2 * LANES
            wide.append(dot(twice, tab[at : at + 2 * LANES, :]) + dot(low, tab[at : at + LANES, :]))
        wide = jnp.concatenate(wide, axis=1)
        index = lax.broadcasted_iota(jnp.int32, (256, 3 * NX), 0)
        middle = (index >= ROWS) & (index < 2 * ROWS)
        rounded = wide.astype(BF16).astype(F32)
        cs[...] = jnp.where(middle, wide - rounded, rounded).astype(BF16)

    def slope(c):
        return g[c].reshape(CHUNK, NX).astype(F32)

    def through():
        field = dot(tab[AT_KD : AT_KD + CHUNK, :], cs[...])
        slopes = [slope(c) for c in range(3)]
        s = slopes[0] * field[:, 0:NX]
        s = s + slopes[1] * field[:, NX : 2 * NX]
        s = s + slopes[2] * field[:, 2 * NX : 3 * NX]
        return slopes, s

    def square_sum(s):
        return fold(jnp.sum((s * s).reshape(CHUNK // 8, 8, NX), axis=0))

    def apply():
        slopes, s = through()
        keep(gather_x([slopes[c] * s for c in range(3)]))
        return square_sum(s)

    def apply_forward():
        unused, s = through()
        along_s[...] = s
        return square_sum(s)

    def apply_back():
        s = along_s[...]
        keep(gather_x([slope(c) * s for c in range(3)]))

    def fold(x):
        total = jnp.sum(x, axis=0, keepdims=True)
        return total[:, 0:LANES] + total[:, LANES : 2 * LANES]

    def tile_sum(x):
        return jnp.sum(jnp.sum(x, axis=0), axis=0, keepdims=True)

    def reduce_start(stage, value):
        me, count = (e, ny) if stage == 0 else (d, nz)
        ars[stage] = value
        arr[stage, me] = value

        for k in sorted(range(1, count), key=lambda k: -min(k, count - k)):
            other = lax.rem(me + k, count)
            z, y = (d, other) if stage == 0 else (other, e)
            remote(ars.at[stage], arr.at[stage, me], ass.at[stage], arsem.at[stage], z, y).start()

    def reduce_end(stage):
        count = ny if stage == 0 else nz
        others = arr.at[stage, pl.ds(0, count - 1)]
        pltpu.make_async_copy(others, others, arsem.at[stage]).wait()
        return jnp.sum(arr[stage, 0:count], axis=0)

    copies0 = exchange(0)
    r0 = collect(0, copies0)
    spread_x(r0)
    energy0 = apply()
    copies1 = exchange(1)
    t = collect(1, copies1)
    spread_x(t)
    energy1 = apply_forward()
    sums = [tile_sum(r0 * r0 * own), energy0, tile_sum(t * t * own), energy1]
    reduce_start(0, jnp.concatenate(sums, axis=0))
    apply_back()
    copies2 = exchange(2)
    reduce_start(1, reduce_end(0))
    t2 = collect(2, copies2)
    total = jnp.sum(reduce_end(1), axis=1, keepdims=True)
    rr0 = total[0:1]
    m1, m2, m3 = (total[k : k + 1] / rr0 for k in (1, 2, 3))
    alpha0 = 1.0 / (m1 + DAMPING)
    beta = alpha0 * alpha0 * (m2 - m1 * m1)
    curve = alpha0 * alpha0 * ((m3 - m1 * m2) - m1 * (m2 - m1 * m1)) + DAMPING * beta
    alpha1 = beta / (curve - beta * beta / alpha0)
    m1, alpha0, alpha1, beta = (x.reshape(1, 1, 1) for x in (m1, alpha0, alpha1, beta))
    r1 = alpha0 * (m1 * r0 - t)
    direction = r1 + beta * r0
    along = alpha0 * (m1 * t - t2) + DAMPING * r1 + beta * (t + DAMPING * r0)
    parts = (alpha0 * r0, alpha1 * direction, r1, -alpha1 * along)
    for k, part in enumerate(parts):
        for c in range(3):
            out[k, c] = part[1 : 1 + CA, 1 : 1 + CB, c * CE : (c + 1) * CE]

    for copy, target in zip(halo + copies0 + copies1 + copies2, (has_up, has_down, has_right, has_left) + targets * 3):
        pl.when(target)(copy.wait_send)
    for stage in range(2):
        others = arr.at[stage, pl.ds(0, (ny if stage == 0 else nz) - 1)]
        pltpu.make_async_copy(others, others, ass.at[stage]).wait()


def solution(mesh):
    nz, ny = mesh.shape["gz"], mesh.shape["gy"]
    tables = constants()
    count = max(nz, ny)
    vmem = pltpu.VMEM
    dma = pltpu.SemaphoreType.DMA
    scratch = [
        vmem((CZ, CY, NX), F32), vmem((CZ, CY, NX), F32),
        vmem((CZ + 6, CY + 16, NX), F32),
        vmem((CZ, 8, NX), F32), vmem((CZ, 8, NX), F32), vmem((CZ, 8, NX), F32), vmem((CZ, 8, NX), F32),
        vmem((CZ, 4, NX), F32), vmem((CZ, 4, NX), F32),
        vmem((3, CY, NX), F32), vmem((3, CY, NX), F32),
        vmem((CZ, 4, NX), F32), vmem((CZ, 4, NX), F32),
        vmem((3, CZ, CY, NX), BF16),
        vmem((CZ * CY, NX), F32),
        vmem((CZ, CY, 2 * LANES), BF16),
        vmem((256, 3 * NX), BF16),
        vmem((256, LANES), F32),
        vmem((A, B, LANES), F32),
        vmem((CZ, CY, LANES), F32),
        vmem((TABLE, NX), BF16),
        vmem((3, A, B, LANES), F32),
        vmem((3, 2, A, 4, LANES), F32),
        vmem((3, 2, 3, B, LANES), F32),
        vmem((3, 2, A, 4, LANES), F32),
        vmem((3, 4, 3, 4, LANES), F32),
        vmem((2, 4, LANES), F32),
        vmem((2, count, 4, LANES), F32),
        dma((12,)), dma((4,)), dma((4,)), dma((3, 8)), dma((3, 8)), dma((2,)), dma((2,)),
    ]
    out = jax.ShapeDtypeStruct((4, 3, CA, CB, CE), F32)
    call = pl.pallas_call(
        functools.partial(kernel, nz, ny),
        out_shape=out,
        in_specs=[pl.BlockSpec(memory_space=pl.ANY)] * 3,
        out_specs=pl.BlockSpec(memory_space=pltpu.VMEM),
        scratch_shapes=scratch,
        compiler_params=pltpu.CompilerParams(collective_id=0, has_side_effects=True, vmem_limit_bytes=VMEM_BYTES),
        name="cg_step",
    )

    def shards(fixed, moving):
        parts = call(fixed, moving, jnp.asarray(tables))
        return parts[0] + parts[1], parts[2] + parts[3]

    return jax.shard_map(
        shards,
        mesh=mesh,
        in_specs=(P("gz", "gy", None), P("gz", "gy", None)),
        out_specs=(P(None, "gz", "gy", None), P(None, "gz", "gy", None)),
        check_vma=False,
    )
```

```python
import functools

import jax
import jax.numpy as jnp
import numpy as np
from jax import lax
from jax.experimental import pallas as pl
from jax.experimental.pallas import tpu as pltpu
from jax.sharding import PartitionSpec as P

SPACING = 8
DAMPING = 8.0
CZ, CY, NX = 32, 64, 256
CA, CB, CE = 4, 8, 32
A, B, LANES = 7, 16, 128
BP = 11
ROWS = 80
CHUNK = CZ * CY
INNER = 8
OUTER = 4
STRIPS = CZ * CY // NX
AT_BXE = NX
AT_BXD = AT_BXE + 3 * NX
AT_KE = AT_BXD + 6 * LANES
AT_KD = AT_KE + 2 * A * B * STRIPS
TABLE = AT_KD + CZ * CY
VMEM_BYTES = 52 * 1024 * 1024
MESH = pl.DeviceIdType.MESH
F32, BF16 = jnp.float32, jnp.bfloat16


def basis_matrix(count, columns, offset):
    voxel = np.arange(count)
    cell = voxel // SPACING
    frac = (voxel % SPACING + 0.5) / SPACING
    other = 1.0 - frac
    weights = (
        other**3 / 6.0,
        (3.0 * frac**3 - 6.0 * frac**2 + 4.0) / 6.0,
        (-3.0 * frac**3 + 3.0 * frac**2 + 3.0 * frac + 1.0) / 6.0,
        frac**3 / 6.0,
    )
    matrix = np.zeros((count, columns))
    for tap in range(4):
        for v in range(count):
            column = cell[v] - 1 + tap + offset
            if 0 <= column < columns:
                matrix[v, column] += weights[tap][v]
    return matrix


def halves(x):
    x = np.asarray(x, np.float32)
    high = x.astype(jnp.bfloat16)
    low = (x - high.astype(np.float32)).astype(jnp.bfloat16)
    return high, low


def constants():
    bz = basis_matrix(CZ, A, 1)
    by = basis_matrix(CY, B, 1)
    bx = basis_matrix(NX, CE, 0)
    narrow = np.einsum("za,yb->zyab", bz, by[:, :BP]).reshape(CZ * CY, A * BP)
    high, low = halves(np.pad(narrow, ((0, 0), (0, ROWS - A * BP))))
    pad = np.zeros((CZ * CY, 256 - 3 * ROWS), jnp.bfloat16)
    kd = np.concatenate([high, high, low, pad], axis=1)
    kron16 = np.einsum("za,yb->abzy", bz, by).reshape(A * B, CZ * CY)
    ke = np.concatenate(halves(kron16), axis=0)
    spread = np.zeros((LANES, 3 * NX))
    for c in range(3):
        spread[c * CE : (c + 1) * CE, c * NX : (c + 1) * NX] = bx.T
    high, low = halves(spread)
    bxd = np.concatenate([high, low], axis=0)
    bxe = np.concatenate([high.T, low.T], axis=1)
    dx = np.zeros((NX, NX))
    for step, weight in ((1, 45.0), (2, -9.0), (3, 1.0)):
        for v in range(NX):
            if v + step < NX:
                dx[v + step, v] = weight
            if v - step >= 0:
                dx[v - step, v] = -weight
    bxd = bxd.reshape(2 * LANES, 3, NX).transpose(1, 0, 2).reshape(6 * LANES, NX)
    ke = ke.reshape(2 * A * B, STRIPS, NX).transpose(1, 0, 2).reshape(2 * A * B * STRIPS, NX)
    return np.concatenate([dx.astype(jnp.bfloat16), bxe, bxd, ke, kd], axis=0)


def split(x):
    high = x.astype(BF16)
    return high, (x - high.astype(F32)).astype(BF16)


def dot(a, b):
    return jnp.dot(a, b, preferred_element_type=F32)


def kernel(nz, ny, fixed, moving, tab_h, out,
           fv, mv, mp, fl, ml, fh, mh, yls, yhs, zlr, zhr, ylr, yhr,
           g, along_s, u, cs, p3, tot, up_x, tab,
           enc, yst, rz, ry, rc, ars, arr,
           lsem, hss, hrs, xss, xrs, ass, arsem):
    d = lax.axis_index("gz")
    e = lax.axis_index("gy")
    up, down = lax.rem(d + 1, nz), lax.rem(d + nz - 1, nz)
    right, left = lax.rem(e + 1, ny), lax.rem(e + ny - 1, ny)

    has_down, has_up, has_left, has_right = d > 0, d < nz - 1, e > 0, e < ny - 1

    def local(k, src, dst):
        copy = pltpu.make_async_copy(src, dst, lsem.at[k])
        copy.start()
        return copy

    faces_z = [
        local(0, fixed.at[pl.ds(0, 3)], fv.at[pl.ds(0, 3)]),
        local(1, moving.at[pl.ds(0, 3)], mv.at[pl.ds(0, 3)]),
        local(2, fixed.at[pl.ds(CZ - 3, 3)], fv.at[pl.ds(CZ - 3, 3)]),
        local(3, moving.at[pl.ds(CZ - 3, 3)], mv.at[pl.ds(CZ - 3, 3)]),
    ]
    faces_y = [
        local(4, fixed.at[:, pl.ds(0, 8)], fl),
        local(5, moving.at[:, pl.ds(0, 8)], ml),
        local(6, fixed.at[:, pl.ds(CY - 8, 8)], fh),
        local(7, moving.at[:, pl.ds(CY - 8, 8)], mh),
    ]
    rest = [
        local(8, fixed.at[pl.ds(3, CZ - 6)], fv.at[pl.ds(3, CZ - 6)]),
        local(9, moving.at[pl.ds(3, CZ - 6)], mv.at[pl.ds(3, CZ - 6)]),
        local(10, tab_h.at[pl.ds(0, 4 * NX)], tab.at[pl.ds(0, 4 * NX)]),
    ]

    barrier = pltpu.get_barrier_semaphore()

    def greet_y(k, carry):
        pl.semaphore_signal(barrier, inc=1, device_id=(d, lax.rem(e + k, ny)), device_id_type=MESH)
        return carry

    def greet_z(k, carry):
        pl.semaphore_signal(barrier, inc=1, device_id=(lax.rem(d + k, nz), e), device_id_type=MESH)
        return carry

    for z in (up, down):
        for y in (right, left):
            pl.semaphore_signal(barrier, inc=1, device_id=(z, y), device_id_type=MESH)
    lax.fori_loop(1, ny, greet_y, 0)
    lax.fori_loop(1, nz, greet_z, 0)

    def clear(missing, refs):
        @pl.when(jnp.logical_not(missing))
        def _():
            for ref in refs:
                ref[...] = jnp.zeros(ref.shape, F32)

    clear(has_down, [zlr] + [rz.at[k, 0] for k in range(3)])
    clear(has_up, [zhr] + [rz.at[k, 1] for k in range(3)])
    clear(has_left, [ylr] + [ry.at[k, 0] for k in range(3)])
    clear(has_right, [yhr] + [ry.at[k, 1] for k in range(3)])
    clear(has_down & has_left, [rc.at[k, 0] for k in range(3)])
    clear(has_down & has_right, [rc.at[k, 1] for k in range(3)])
    clear(has_up & has_left, [rc.at[k, 2] for k in range(3)])
    clear(has_up & has_right, [rc.at[k, 3] for k in range(3)])

    def remote(src, dst, send, recv, z, y):
        return pltpu.make_async_remote_copy(
            src_ref=src, dst_ref=dst, send_sem=send, recv_sem=recv, device_id=(z, y), device_id_type=MESH
        )

    for copy in faces_z:
        copy.wait()
    for z in (0, 1, 2, CZ - 3, CZ - 2, CZ - 1):
        mp[z + 3, 8 : 8 + CY, :] = 0.5 * (fv[z] + mv[z])
    pl.semaphore_wait(barrier, 4 + (ny - 1) + (nz - 1))
    halo = [
        remote(mp.at[pl.ds(CZ, 3), pl.ds(8, CY)], zlr, hss.at[0], hrs.at[0], up, e),
        remote(mp.at[pl.ds(3, 3), pl.ds(8, CY)], zhr, hss.at[1], hrs.at[1], down, e),
        remote(yhs, ylr, hss.at[2], hrs.at[2], d, right),
        remote(yls, yhr, hss.at[3], hrs.at[3], d, left),
    ]
    pl.when(has_up)(halo[0].start)
    pl.when(has_down)(halo[1].start)
    for copy in faces_y:
        copy.wait()
    yls[...] = 0.5 * (fl[:, 0:4, :] + ml[:, 0:4, :])
    yhs[...] = 0.5 * (fh[:, 4:8, :] + mh[:, 4:8, :])
    pl.when(has_right)(halo[2].start)
    pl.when(has_left)(halo[3].start)
    p3[...] = jnp.zeros_like(p3)
    cs[3 * ROWS : 256, :] = jnp.zeros((256 - 3 * ROWS, 3 * NX), BF16)

    for copy in rest:
        copy.wait()
    tail = pl.ds(4 * NX, TABLE - 4 * NX)
    later = [local(11, tab_h.at[tail], tab.at[tail])]

    def fill(z, carry):
        mp[z + 3, 8 : 8 + CY, :] = 0.5 * (fv[z] + mv[z])
        return carry

    lax.fori_loop(3, CZ - 3, fill, 0)

    def gather_x(volume):
        total = None
        for c in range(3):
            if volume[c] is None:
                continue
            term = dot(volume[c].astype(BF16), tab[AT_BXE + c * NX : AT_BXE + (c + 1) * NX, :])
            total = term if total is None else total + term
        return total[:, :LANES] + total[:, LANES:]

    def keep(total):
        high, low = split(total)
        u[...] = jnp.concatenate([high, low], axis=1).reshape(CZ, CY, 2 * LANES)

    edges, middle, every = ((0, 16), (CY - 16, 16)), ((16, CY - 32),), ((0, CY),)

    def first(z, layers, spans, parts, begun, done):
        count = layers * sum(size for unused, size in spans)
        deep = pl.ds(z, layers)

        def block(ref, dz, dy):
            pieces = [ref[pl.ds(z + dz, layers), dy + y : dy + y + size, :] for y, size in spans]
            whole = pieces[0] if len(pieces) == 1 else jnp.concatenate(pieces, axis=1)
            return whole.reshape(count, whole.shape[-1])

        def put(ref, value):
            value = value.reshape(layers, -1, value.shape[-1])
            at = 0
            for y, size in spans:
                ref[deep, y : y + size, :] = value[:, at : at + size]
                at += size

        def difference(part):
            return 45.0 * (part(1) - part(-1)) - 9.0 * (part(2) - part(-2)) + (part(3) - part(-3))

        mismatch = block(fv, 0, 0) - block(mv, 0, 0)
        volume = [None] * 3
        for c in parts:
            if c == 0:
                slope = difference(lambda k: block(mp, 3 + k, 8))
            elif c == 1:
                slope = difference(lambda k: block(mp, 3, 8 + k))
            else:
                high, low = split(block(mp, 3, 8))
                slope = dot(high, tab[0:NX, :]) + dot(low, tab[0:NX, :])
            rounded = (slope * (1.0 / 60.0)).astype(BF16)
            put(g.at[c], rounded)
            volume[c] = rounded.astype(F32) * mismatch
        total = gather_x(volume)
        if begun:
            total = total + block(up_x, 0, 0)
        if not done:
            put(up_x, total)
        else:
            high, low = split(total)
            put(u, jnp.concatenate([high, low], axis=1))

    inner, faces = (CZ - 2 * OUTER) // INNER, CZ - OUTER

    def own_inner(t, carry):
        first(OUTER + t * INNER, INNER, middle, (0, 1, 2), False, True)
        first(OUTER + t * INNER, INNER, edges, (0, 2), False, False)
        return carry

    def own_outer(t, carry):
        first(t * faces, OUTER, every, (2,), False, False)
        return carry

    def side_inner(t, carry):
        first(OUTER + t * INNER, INNER, edges, (1,), True, True)
        return carry

    def side_outer(t, carry):
        first(t * faces, OUTER, every, (1,), True, False)
        return carry

    def top_outer(t, carry):
        first(t * faces, OUTER, every, (0,), True, True)
        return carry

    lax.fori_loop(0, inner, own_inner, 0)
    lax.fori_loop(0, 2, own_outer, 0)
    pl.when(has_left)(halo[2].wait_recv)
    mp[3 : CZ + 3, 4:8, :] = ylr[...]
    pl.when(has_right)(halo[3].wait_recv)
    mp[3 : CZ + 3, 8 + CY : 12 + CY, :] = yhr[...]

    lax.fori_loop(0, inner, side_inner, 0)
    lax.fori_loop(0, 2, side_outer, 0)
    pl.when(has_down)(halo[0].wait_recv)
    mp[0:3, 8 : 8 + CY, :] = zlr[...]
    pl.when(has_up)(halo[1].wait_recv)
    mp[CZ + 3 : CZ + 6, 8 : 8 + CY, :] = zhr[...]
    lax.fori_loop(0, 2, top_outer, 0)
    for copy in later:
        copy.wait()

    row = lax.broadcasted_iota(jnp.int32, (1, 4, LANES), 1)
    low_rows = jnp.where(row < 3, 1.0, 0.0).astype(F32)
    pa = lax.broadcasted_iota(jnp.int32, (A, B, LANES), 0) + (d * CA - 1)
    pb = lax.broadcasted_iota(jnp.int32, (A, B, LANES), 1) + (e * CB - 1)
    ia = lax.broadcasted_iota(jnp.int32, (A, B, LANES), 0)
    ib = lax.broadcasted_iota(jnp.int32, (A, B, LANES), 1)
    inside = (pa >= 0) & (pa < nz * CA) & (pb >= 0) & (pb < ny * CB) & (ib < 11)
    inside = jnp.where(inside, 1.0, 0.0).astype(F32)
    own = jnp.where((ia >= 1) & (ia < 1 + CA) & (ib >= 1) & (ib < 1 + CB), 1.0, 0.0).astype(F32)

    targets = (has_up & has_right, has_up & has_left, has_down & has_right, has_down & has_left,
               has_up, has_down, has_right, has_left)
    sources = (has_down & has_left, has_down & has_right, has_up & has_left, has_up & has_right,
               has_down, has_up, has_left, has_right)

    def exchange(k):
        half = A * B
        both = None
        for n in range(STRIPS):
            strip = tab[AT_KE + n * 2 * half : AT_KE + (n + 1) * 2 * half, :]
            layers = NX // CY
            term = dot(strip, u[n * layers : (n + 1) * layers].reshape(NX, 2 * LANES))
            both = term if both is None else both + term
        total = both[:half, :LANES] + both[half:, :LANES] + both[:half, LANES:]
        total = total.reshape(A, B, LANES)
        enc[k] = total
        yst[k, 0] = total[:, 8:12]
        yst[k, 1] = total[:, 0:4]
        src, after, before = enc.at[k], yst.at[k, 0], yst.at[k, 1]
        top, bottom = pl.ds(A - 3, 3), pl.ds(0, 3)
        copies = [
            remote(after.at[top], rc.at[k, 0], xss.at[k, 0], xrs.at[k, 0], up, right),
            remote(before.at[top], rc.at[k, 1], xss.at[k, 1], xrs.at[k, 1], up, left),
            remote(after.at[bottom], rc.at[k, 2], xss.at[k, 2], xrs.at[k, 2], down, right),
            remote(before.at[bottom], rc.at[k, 3], xss.at[k, 3], xrs.at[k, 3], down, left),
            remote(src.at[top], rz.at[k, 0], xss.at[k, 4], xrs.at[k, 4], up, e),
            remote(src.at[bottom], rz.at[k, 1], xss.at[k, 5], xrs.at[k, 5], down, e),
            remote(after, ry.at[k, 0], xss.at[k, 6], xrs.at[k, 6], d, right),
            remote(before, ry.at[k, 1], xss.at[k, 7], xrs.at[k, 7], d, left),
        ]
        for copy, target in zip(copies, targets):
            pl.when(target)(copy.start)
        return copies

    def collect(k, copies):
        for copy, source in zip(copies, sources):
            pl.when(source)(copy.wait_recv)
        tot[...] = enc[k]
        tot[0:3] += rz[k, 0]
        tot[4:7] += rz[k, 1]
        tot[:, 0:4] += ry[k, 0]
        tot[:, 8:12] += low_rows * ry[k, 1]
        tot[0:3, 0:4] += rc[k, 0]
        tot[0:3, 8:12] += low_rows * rc[k, 1]
        tot[4:7, 0:4] += rc[k, 2]
        tot[4:7, 8:12] += low_rows * rc[k, 3]
        return tot[...] * inside

    def spread_x(control):
        for a in range(A):
            p3[a * BP : (a + 1) * BP, :] = control[a, 0:BP, :]
        high, low = split(p3[...])
        twice = jnp.concatenate([high, high], axis=1)
        wide = []
        for c in range(3):
            at = AT_BXD + c * 2 * LANES
            wide.append(dot(twice, tab[at : at + 2 * LANES, :]) + dot(low, tab[at : at + LANES, :]))
        high, low = split(jnp.concatenate(wide, axis=1))
        cs[0:ROWS, :] = high
        cs[ROWS : 2 * ROWS, :] = low
        cs[2 * ROWS : 3 * ROWS, :] = high

    def slope(c):
        return g[c].reshape(CHUNK, NX).astype(F32)

    def through():
        field = dot(tab[AT_KD : AT_KD + CHUNK, :], cs[...])
        slopes = [slope(c) for c in range(3)]
        s = slopes[0] * field[:, 0:NX]
        s = s + slopes[1] * field[:, NX : 2 * NX]
        s = s + slopes[2] * field[:, 2 * NX : 3 * NX]
        return slopes, s

    def square_sum(s):
        return fold(jnp.sum((s * s).reshape(CHUNK // 8, 8, NX), axis=0))

    def apply():
        slopes, s = through()
        keep(gather_x([slopes[c] * s for c in range(3)]))
        return square_sum(s)

    def apply_forward():
        unused, s = through()
        along_s[...] = s
        return square_sum(s)

    def apply_back():
        s = along_s[...]
        keep(gather_x([slope(c) * s for c in range(3)]))

    def fold(x):
        total = jnp.sum(x, axis=0, keepdims=True)
        return total[:, 0:LANES] + total[:, LANES : 2 * LANES]

    def tile_sum(x):
        return jnp.sum(jnp.sum(x, axis=0), axis=0, keepdims=True)

    def reduce_start(stage, value):
        me, count = (e, ny) if stage == 0 else (d, nz)
        ars[stage] = value
        arr[stage, me] = value

        for k in sorted(range(1, count), key=lambda k: -min(k, count - k)):
            other = lax.rem(me + k, count)
            z, y = (d, other) if stage == 0 else (other, e)
            remote(ars.at[stage], arr.at[stage, me], ass.at[stage], arsem.at[stage], z, y).start()

    def reduce_end(stage):
        count = ny if stage == 0 else nz
        others = arr.at[stage, pl.ds(0, count - 1)]
        pltpu.make_async_copy(others, others, arsem.at[stage]).wait()
        return jnp.sum(arr[stage, 0:count], axis=0)

    copies0 = exchange(0)
    r0 = collect(0, copies0)
    spread_x(r0)
    square0 = tile_sum(r0 * r0 * own)
    energy0 = apply()
    copies1 = exchange(1)
    t = collect(1, copies1)
    spread_x(t)
    square1 = tile_sum(t * t * own)
    sums = [square0, energy0, square1, apply_forward()]
    reduce_start(0, jnp.concatenate(sums, axis=0))
    apply_back()
    copies2 = exchange(2)
    reduce_start(1, reduce_end(0))
    t2 = collect(2, copies2)
    total = jnp.sum(reduce_end(1), axis=1, keepdims=True)
    rr0 = total[0:1]
    m1, m2, m3 = (total[k : k + 1] / rr0 for k in (1, 2, 3))
    alpha0 = 1.0 / (m1 + DAMPING)
    beta = alpha0 * alpha0 * (m2 - m1 * m1)
    curve = alpha0 * alpha0 * ((m3 - m1 * m2) - m1 * (m2 - m1 * m1)) + DAMPING * beta
    alpha1 = beta / (curve - beta * beta / alpha0)
    m1, alpha0, alpha1, beta = (x.reshape(1, 1, 1) for x in (m1, alpha0, alpha1, beta))
    r1 = alpha0 * (m1 * r0 - t)
    direction = r1 + beta * r0
    along = alpha0 * (m1 * t - t2) + DAMPING * r1 + beta * (t + DAMPING * r0)
    parts = (alpha0 * r0, alpha1 * direction, r1, -alpha1 * along)
    for k, part in enumerate(parts):
        for c in range(3):
            out[k, c] = part[1 : 1 + CA, 1 : 1 + CB, c * CE : (c + 1) * CE]

    for copy, target in zip(halo + copies0 + copies1 + copies2, (has_up, has_down, has_right, has_left) + targets * 3):
        pl.when(target)(copy.wait_send)
    for stage in range(2):
        others = arr.at[stage, pl.ds(0, (ny if stage == 0 else nz) - 1)]
        pltpu.make_async_copy(others, others, ass.at[stage]).wait()


def solution(mesh):
    nz, ny = mesh.shape["gz"], mesh.shape["gy"]
    tables = constants()
    count = max(nz, ny)
    vmem = pltpu.VMEM
    dma = pltpu.SemaphoreType.DMA
    scratch = [
        vmem((CZ, CY, NX), F32), vmem((CZ, CY, NX), F32),
        vmem((CZ + 6, CY + 16, NX), F32),
        vmem((CZ, 8, NX), F32), vmem((CZ, 8, NX), F32), vmem((CZ, 8, NX), F32), vmem((CZ, 8, NX), F32),
        vmem((CZ, 4, NX), F32), vmem((CZ, 4, NX), F32),
        vmem((3, CY, NX), F32), vmem((3, CY, NX), F32),
        vmem((CZ, 4, NX), F32), vmem((CZ, 4, NX), F32),
        vmem((3, CZ, CY, NX), BF16),
        vmem((CZ * CY, NX), F32),
        vmem((CZ, CY, 2 * LANES), BF16),
        vmem((256, 3 * NX), BF16),
        vmem((ROWS, LANES), F32),
        vmem((A, B, LANES), F32),
        vmem((CZ, CY, LANES), F32),
        vmem((TABLE, NX), BF16),
        vmem((3, A, B, LANES), F32),
        vmem((3, 2, A, 4, LANES), F32),
        vmem((3, 2, 3, B, LANES), F32),
        vmem((3, 2, A, 4, LANES), F32),
        vmem((3, 4, 3, 4, LANES), F32),
        vmem((2, 4, LANES), F32),
        vmem((2, count, 4, LANES), F32),
        dma((12,)), dma((4,)), dma((4,)), dma((3, 8)), dma((3, 8)), dma((2,)), dma((2,)),
    ]
    out = jax.ShapeDtypeStruct((4, 3, CA, CB, CE), F32)
    call = pl.pallas_call(
        functools.partial(kernel, nz, ny),
        out_shape=out,
        in_specs=[pl.BlockSpec(memory_space=pl.ANY)] * 3,
        out_specs=pl.BlockSpec(memory_space=pltpu.VMEM),
        scratch_shapes=scratch,
        compiler_params=pltpu.CompilerParams(collective_id=0, has_side_effects=True, vmem_limit_bytes=VMEM_BYTES),
        name="cg_step",
    )

    def shards(fixed, moving):
        parts = call(fixed, moving, jnp.asarray(tables))
        return parts[0] + parts[1], parts[2] + parts[3]

    return jax.shard_map(
        shards,
        mesh=mesh,
        in_specs=(P("gz", "gy", None), P("gz", "gy", None)),
        out_specs=(P(None, "gz", "gy", None), P(None, "gz", "gy", None)),
        check_vma=False,
    )
```

```python
import functools

import jax
import jax.numpy as jnp
import numpy as np
from jax import lax
from jax.experimental import pallas as pl
from jax.experimental.pallas import tpu as pltpu
from jax.sharding import PartitionSpec as P

SPACING = 8
DAMPING = 8.0
CZ, CY, NX = 32, 64, 256
CA, CB, CE = 4, 8, 32
A, B, LANES = 7, 16, 128
BP = 11
ROWS = 80
DEEP = 8
CHUNK = DEEP * CY
INNER = 8
OUTER = 4
STRIPS = CZ * CY // NX
AT_BXE = NX
AT_BXD = AT_BXE + 3 * NX
AT_KE = AT_BXD + 6 * LANES
AT_KD = AT_KE + 2 * A * B * STRIPS
TABLE = AT_KD + CZ * CY
VMEM_BYTES = 52 * 1024 * 1024
MESH = pl.DeviceIdType.MESH
F32, BF16 = jnp.float32, jnp.bfloat16


def basis_matrix(count, columns, offset):
    voxel = np.arange(count)
    cell = voxel // SPACING
    frac = (voxel % SPACING + 0.5) / SPACING
    other = 1.0 - frac
    weights = (
        other**3 / 6.0,
        (3.0 * frac**3 - 6.0 * frac**2 + 4.0) / 6.0,
        (-3.0 * frac**3 + 3.0 * frac**2 + 3.0 * frac + 1.0) / 6.0,
        frac**3 / 6.0,
    )
    matrix = np.zeros((count, columns))
    for tap in range(4):
        for v in range(count):
            column = cell[v] - 1 + tap + offset
            if 0 <= column < columns:
                matrix[v, column] += weights[tap][v]
    return matrix


def halves(x):
    x = np.asarray(x, np.float32)
    high = x.astype(jnp.bfloat16)
    low = (x - high.astype(np.float32)).astype(jnp.bfloat16)
    return high, low


def constants():
    bz = basis_matrix(CZ, A, 1)
    by = basis_matrix(CY, B, 1)
    bx = basis_matrix(NX, CE, 0)
    narrow = np.einsum("za,yb->zyab", bz, by[:, :BP]).reshape(CZ * CY, A * BP)
    high, low = halves(np.pad(narrow, ((0, 0), (0, ROWS - A * BP))))
    pad = np.zeros((CZ * CY, 256 - 3 * ROWS), jnp.bfloat16)
    kd = np.concatenate([high, high, low, pad], axis=1)
    kron16 = np.einsum("za,yb->abzy", bz, by).reshape(A * B, CZ * CY)
    ke = np.concatenate(halves(kron16), axis=0)
    spread = np.zeros((LANES, 3 * NX))
    for c in range(3):
        spread[c * CE : (c + 1) * CE, c * NX : (c + 1) * NX] = bx.T
    high, low = halves(spread)
    bxd = np.concatenate([high, low], axis=0)
    bxe = np.concatenate([high.T, low.T], axis=1)
    dx = np.zeros((NX, NX))
    for step, weight in ((1, 45.0), (2, -9.0), (3, 1.0)):
        for v in range(NX):
            if v + step < NX:
                dx[v + step, v] = weight
            if v - step >= 0:
                dx[v - step, v] = -weight
    bxd = bxd.reshape(2 * LANES, 3, NX).transpose(1, 0, 2).reshape(6 * LANES, NX)
    ke = ke.reshape(2 * A * B, STRIPS, NX).transpose(1, 0, 2).reshape(2 * A * B * STRIPS, NX)
    return np.concatenate([dx.astype(jnp.bfloat16), bxe, bxd, ke, kd], axis=0)


def split(x):
    high = x.astype(BF16)
    return high, (x - high.astype(F32)).astype(BF16)


def dot(a, b):
    return jnp.dot(a, b, preferred_element_type=F32)


def kernel(nz, ny, fixed, moving, tab_h, out,
           fv, mv, mp, fl, ml, fh, mh, yls, yhs, zlr, zhr, ylr, yhr,
           g, along_s, u, cs, p3, tot, up_x, tab,
           enc, yst, rz, ry, rc, ars, arr,
           lsem, hss, hrs, xss, xrs, ass, arsem):
    d = lax.axis_index("gz")
    e = lax.axis_index("gy")
    up, down = lax.rem(d + 1, nz), lax.rem(d + nz - 1, nz)
    right, left = lax.rem(e + 1, ny), lax.rem(e + ny - 1, ny)

    has_down, has_up, has_left, has_right = d > 0, d < nz - 1, e > 0, e < ny - 1

    def local(k, src, dst):
        copy = pltpu.make_async_copy(src, dst, lsem.at[k])
        copy.start()
        return copy

    faces_z = [
        local(0, fixed.at[pl.ds(0, 3)], fv.at[pl.ds(0, 3)]),
        local(1, moving.at[pl.ds(0, 3)], mv.at[pl.ds(0, 3)]),
        local(2, fixed.at[pl.ds(CZ - 3, 3)], fv.at[pl.ds(CZ - 3, 3)]),
        local(3, moving.at[pl.ds(CZ - 3, 3)], mv.at[pl.ds(CZ - 3, 3)]),
    ]
    faces_y = [
        local(4, fixed.at[:, pl.ds(0, 8)], fl),
        local(5, moving.at[:, pl.ds(0, 8)], ml),
        local(6, fixed.at[:, pl.ds(CY - 8, 8)], fh),
        local(7, moving.at[:, pl.ds(CY - 8, 8)], mh),
    ]
    rest = [
        local(8, fixed.at[pl.ds(3, CZ - 6)], fv.at[pl.ds(3, CZ - 6)]),
        local(9, moving.at[pl.ds(3, CZ - 6)], mv.at[pl.ds(3, CZ - 6)]),
        local(10, tab_h.at[pl.ds(0, 4 * NX)], tab.at[pl.ds(0, 4 * NX)]),
    ]

    barrier = pltpu.get_barrier_semaphore()

    near = [(up, e), (down, e), (d, right), (d, left), (up, right), (up, left), (down, right), (down, left)]
    far = [(d, lax.rem(e + k, ny)) for k in range(2, ny - 1)] + [(lax.rem(d + k, nz), e) for k in range(2, nz - 1)]
    for target in near + far:
        pl.semaphore_signal(barrier, inc=1, device_id=target, device_id_type=MESH)

    def clear(missing, refs):
        @pl.when(jnp.logical_not(missing))
        def _():
            for ref in refs:
                ref[...] = jnp.zeros(ref.shape, F32)

    clear(has_down, [zlr] + [rz.at[k, 0] for k in range(3)])
    clear(has_up, [zhr] + [rz.at[k, 1] for k in range(3)])
    clear(has_left, [ylr] + [ry.at[k, 0] for k in range(3)])
    clear(has_right, [yhr] + [ry.at[k, 1] for k in range(3)])
    clear(has_down & has_left, [rc.at[k, 0] for k in range(3)])
    clear(has_down & has_right, [rc.at[k, 1] for k in range(3)])
    clear(has_up & has_left, [rc.at[k, 2] for k in range(3)])
    clear(has_up & has_right, [rc.at[k, 3] for k in range(3)])

    def remote(src, dst, send, recv, z, y):
        return pltpu.make_async_remote_copy(
            src_ref=src, dst_ref=dst, send_sem=send, recv_sem=recv, device_id=(z, y), device_id_type=MESH
        )

    for copy in faces_z:
        copy.wait()
    for z in (0, 1, 2, CZ - 3, CZ - 2, CZ - 1):
        mp[z + 3, 8 : 8 + CY, :] = 0.5 * (fv[z] + mv[z])
    pl.semaphore_wait(barrier, 4 + (ny - 1) + (nz - 1))
    halo = [
        remote(mp.at[pl.ds(CZ, 3), pl.ds(8, CY)], zlr, hss.at[0], hrs.at[0], up, e),
        remote(mp.at[pl.ds(3, 3), pl.ds(8, CY)], zhr, hss.at[1], hrs.at[1], down, e),
        remote(yhs, ylr, hss.at[2], hrs.at[2], d, right),
        remote(yls, yhr, hss.at[3], hrs.at[3], d, left),
    ]
    pl.when(has_up)(halo[0].start)
    pl.when(has_down)(halo[1].start)
    for copy in faces_y:
        copy.wait()
    yls[...] = 0.5 * (fl[:, 0:4, :] + ml[:, 0:4, :])
    yhs[...] = 0.5 * (fh[:, 4:8, :] + mh[:, 4:8, :])
    pl.when(has_right)(halo[2].start)
    pl.when(has_left)(halo[3].start)
    p3[...] = jnp.zeros_like(p3)
    cs[3 * ROWS : 256, :] = jnp.zeros((256 - 3 * ROWS, 3 * NX), BF16)

    for copy in rest:
        copy.wait()
    tail = pl.ds(4 * NX, TABLE - 4 * NX)
    later = [local(11, tab_h.at[tail], tab.at[tail])]

    def fill(z, carry):
        mp[z + 3, 8 : 8 + CY, :] = 0.5 * (fv[z] + mv[z])
        return carry

    lax.fori_loop(3, CZ - 3, fill, 0)

    def gather_x(volume):
        total = None
        for c in range(3):
            if volume[c] is None:
                continue
            term = dot(volume[c].astype(BF16), tab[AT_BXE + c * NX : AT_BXE + (c + 1) * NX, :])
            total = term if total is None else total + term
        return total[:, :LANES] + total[:, LANES:]

    edges, middle, every = ((0, 16), (CY - 16, 16)), ((16, CY - 32),), ((0, CY),)

    def first(z, layers, spans, parts, begun, done):
        count = layers * sum(size for unused, size in spans)
        deep = pl.ds(z, layers)

        def block(ref, dz, dy):
            pieces = [ref[pl.ds(z + dz, layers), dy + y : dy + y + size, :] for y, size in spans]
            whole = pieces[0] if len(pieces) == 1 else jnp.concatenate(pieces, axis=1)
            return whole.reshape(count, whole.shape[-1])

        def put(ref, value):
            value = value.reshape(layers, -1, value.shape[-1])
            at = 0
            for y, size in spans:
                ref[deep, y : y + size, :] = value[:, at : at + size]
                at += size

        def difference(part):
            return 45.0 * (part(1) - part(-1)) - 9.0 * (part(2) - part(-2)) + (part(3) - part(-3))

        mismatch = block(fv, 0, 0) - block(mv, 0, 0)
        volume = [None] * 3
        for c in parts:
            if c == 0:
                slope = difference(lambda k: block(mp, 3 + k, 8))
            elif c == 1:
                slope = difference(lambda k: block(mp, 3, 8 + k))
            else:
                high, low = split(block(mp, 3, 8))
                slope = dot(high, tab[0:NX, :]) + dot(low, tab[0:NX, :])
            rounded = (slope * (1.0 / 60.0)).astype(BF16)
            put(g.at[c], rounded)
            volume[c] = rounded.astype(F32) * mismatch
        total = gather_x(volume)
        if begun:
            total = total + block(up_x, 0, 0)
        if not done:
            put(up_x, total)
        else:
            high, low = split(total)
            put(u, jnp.concatenate([high, low], axis=1))

    inner, faces = (CZ - 2 * OUTER) // INNER, CZ - OUTER

    def own_inner(t, carry):
        first(OUTER + t * INNER, INNER, middle, (0, 1, 2), False, True)
        first(OUTER + t * INNER, INNER, edges, (0, 2), False, False)
        return carry

    def own_outer(t, carry):
        first(t * faces, OUTER, every, (2,), False, False)
        return carry

    def side_inner(t, carry):
        first(OUTER + t * INNER, INNER, edges, (1,), True, True)
        return carry

    def side_outer(t, carry):
        first(t * faces, OUTER, every, (1,), True, False)
        return carry

    def top_outer(t, carry):
        first(t * faces, OUTER, every, (0,), True, True)
        return carry

    lax.fori_loop(0, inner, own_inner, 0)
    lax.fori_loop(0, 2, own_outer, 0)
    pl.when(has_left)(halo[2].wait_recv)
    mp[3 : CZ + 3, 4:8, :] = ylr[...]
    pl.when(has_right)(halo[3].wait_recv)
    mp[3 : CZ + 3, 8 + CY : 12 + CY, :] = yhr[...]

    lax.fori_loop(0, inner, side_inner, 0)
    lax.fori_loop(0, 2, side_outer, 0)
    pl.when(has_down)(halo[0].wait_recv)
    mp[0:3, 8 : 8 + CY, :] = zlr[...]
    pl.when(has_up)(halo[1].wait_recv)
    mp[CZ + 3 : CZ + 6, 8 : 8 + CY, :] = zhr[...]
    lax.fori_loop(0, 2, top_outer, 0)
    for copy in later:
        copy.wait()

    row = lax.broadcasted_iota(jnp.int32, (1, 4, LANES), 1)
    low_rows = jnp.where(row < 3, 1.0, 0.0).astype(F32)
    pa = lax.broadcasted_iota(jnp.int32, (A, B, LANES), 0) + (d * CA - 1)
    pb = lax.broadcasted_iota(jnp.int32, (A, B, LANES), 1) + (e * CB - 1)
    ia = lax.broadcasted_iota(jnp.int32, (A, B, LANES), 0)
    ib = lax.broadcasted_iota(jnp.int32, (A, B, LANES), 1)
    inside = (pa >= 0) & (pa < nz * CA) & (pb >= 0) & (pb < ny * CB) & (ib < 11)
    inside = jnp.where(inside, 1.0, 0.0).astype(F32)
    own = jnp.where((ia >= 1) & (ia < 1 + CA) & (ib >= 1) & (ib < 1 + CB), 1.0, 0.0).astype(F32)

    targets = (has_up & has_right, has_up & has_left, has_down & has_right, has_down & has_left,
               has_up, has_down, has_right, has_left)
    sources = (has_down & has_left, has_down & has_right, has_up & has_left, has_up & has_right,
               has_down, has_up, has_left, has_right)

    def exchange(k):
        half = A * B
        both = None
        for n in range(STRIPS):
            strip = tab[AT_KE + n * 2 * half : AT_KE + (n + 1) * 2 * half, :]
            layers = NX // CY
            term = dot(strip, u[n * layers : (n + 1) * layers].reshape(NX, 2 * LANES))
            both = term if both is None else both + term
        total = both[:half, :LANES] + both[half:, :LANES] + both[:half, LANES:]
        total = total.reshape(A, B, LANES)
        enc[k] = total
        yst[k, 0] = total[:, 8:12]
        yst[k, 1] = total[:, 0:4]
        src, after, before = enc.at[k], yst.at[k, 0], yst.at[k, 1]
        top, bottom = pl.ds(A - 3, 3), pl.ds(0, 3)
        copies = [
            remote(after.at[top], rc.at[k, 0], xss.at[k, 0], xrs.at[k, 0], up, right),
            remote(before.at[top], rc.at[k, 1], xss.at[k, 1], xrs.at[k, 1], up, left),
            remote(after.at[bottom], rc.at[k, 2], xss.at[k, 2], xrs.at[k, 2], down, right),
            remote(before.at[bottom], rc.at[k, 3], xss.at[k, 3], xrs.at[k, 3], down, left),
            remote(src.at[top], rz.at[k, 0], xss.at[k, 4], xrs.at[k, 4], up, e),
            remote(src.at[bottom], rz.at[k, 1], xss.at[k, 5], xrs.at[k, 5], down, e),
            remote(after, ry.at[k, 0], xss.at[k, 6], xrs.at[k, 6], d, right),
            remote(before, ry.at[k, 1], xss.at[k, 7], xrs.at[k, 7], d, left),
        ]
        for copy, target in zip(copies, targets):
            pl.when(target)(copy.start)
        return copies

    def collect(k, copies):
        for copy, source in zip(copies, sources):
            pl.when(source)(copy.wait_recv)
        tot[...] = enc[k]
        tot[0:3] += rz[k, 0]
        tot[4:7] += rz[k, 1]
        tot[:, 0:4] += ry[k, 0]
        tot[:, 8:12] += low_rows * ry[k, 1]
        tot[0:3, 0:4] += rc[k, 0]
        tot[0:3, 8:12] += low_rows * rc[k, 1]
        tot[4:7, 0:4] += rc[k, 2]
        tot[4:7, 8:12] += low_rows * rc[k, 3]
        return tot[...] * inside

    def spread_x(control):
        for a in range(A):
            p3[a * BP : (a + 1) * BP, :] = control[a, 0:BP, :]
        high, low = split(p3[...])
        twice = jnp.concatenate([high, high], axis=1)
        wide = []
        for c in range(3):
            at = AT_BXD + c * 2 * LANES
            wide.append(dot(twice, tab[at : at + 2 * LANES, :]) + dot(low, tab[at : at + LANES, :]))
        high, low = split(jnp.concatenate(wide, axis=1))
        cs[0:ROWS, :] = high
        cs[ROWS : 2 * ROWS, :] = low
        cs[2 * ROWS : 3 * ROWS, :] = high

    def strip_of(i):
        return slice(i * DEEP, (i + 1) * DEEP), slice(i * CHUNK, (i + 1) * CHUNK)

    def decode(i):
        unused, rows = strip_of(i)
        weights = tab[AT_KD + i * CHUNK : AT_KD + (i + 1) * CHUNK, :]
        return [dot(weights, cs[:, c * NX : (c + 1) * NX]) for c in range(3)]

    def slopes_of(i):
        deep, unused = strip_of(i)
        return [g[c, deep].reshape(CHUNK, NX).astype(F32) for c in range(3)]

    def along(i):
        field, slopes = decode(i), slopes_of(i)
        s = slopes[0] * field[0] + slopes[1] * field[1] + slopes[2] * field[2]
        return slopes, s, jnp.sum((s * s).reshape(CHUNK // 8, 8, NX), axis=0)

    def keep(i, slopes, s):
        deep, unused = strip_of(i)
        high, low = split(gather_x([slopes[c] * s for c in range(3)]))
        u[deep] = jnp.concatenate([high, low], axis=1).reshape(DEEP, CY, 2 * LANES)

    def apply():
        total = jnp.zeros((8, NX), F32)
        for i in range(CZ // DEEP):
            slopes, s, square = along(i)
            keep(i, slopes, s)
            total = total + square
        return fold(total)

    def apply_forward():
        total = jnp.zeros((8, NX), F32)
        for i in range(CZ // DEEP):
            unused, rows = strip_of(i)
            unused, s, square = along(i)
            along_s[rows, :] = s
            total = total + square
        return fold(total)

    def apply_back():
        for i in range(CZ // DEEP):
            unused, rows = strip_of(i)
            keep(i, slopes_of(i), along_s[rows, :])

    def fold(x):
        total = jnp.sum(x, axis=0, keepdims=True)
        return total[:, 0:LANES] + total[:, LANES : 2 * LANES]

    def tile_sum(x):
        return jnp.sum(jnp.sum(x, axis=0), axis=0, keepdims=True)

    def reduce_start(stage, value):
        me, count = (e, ny) if stage == 0 else (d, nz)
        ars[stage] = value
        arr[stage, me] = value

        for k in sorted(range(1, count), key=lambda k: -min(k, count - k)):
            other = lax.rem(me + k, count)
            z, y = (d, other) if stage == 0 else (other, e)
            remote(ars.at[stage], arr.at[stage, me], ass.at[stage], arsem.at[stage], z, y).start()

    def reduce_end(stage):
        count = ny if stage == 0 else nz
        others = arr.at[stage, pl.ds(0, count - 1)]
        pltpu.make_async_copy(others, others, arsem.at[stage]).wait()
        return jnp.sum(arr[stage, 0:count], axis=0)

    copies0 = exchange(0)
    r0 = collect(0, copies0)
    spread_x(r0)
    square0 = tile_sum(r0 * r0 * own)
    energy0 = apply()
    copies1 = exchange(1)
    t = collect(1, copies1)
    spread_x(t)
    square1 = tile_sum(t * t * own)
    sums = [square0, energy0, square1, apply_forward()]
    reduce_start(0, jnp.concatenate(sums, axis=0))
    apply_back()
    copies2 = exchange(2)
    reduce_start(1, reduce_end(0))
    t2 = collect(2, copies2)
    total = jnp.sum(reduce_end(1), axis=1, keepdims=True)
    rr0 = total[0:1]
    m1, m2, m3 = (total[k : k + 1] / rr0 for k in (1, 2, 3))
    alpha0 = 1.0 / (m1 + DAMPING)
    beta = alpha0 * alpha0 * (m2 - m1 * m1)
    curve = alpha0 * alpha0 * ((m3 - m1 * m2) - m1 * (m2 - m1 * m1)) + DAMPING * beta
    alpha1 = beta / (curve - beta * beta / alpha0)
    m1, alpha0, alpha1, beta = (x.reshape(1, 1, 1) for x in (m1, alpha0, alpha1, beta))
    r1 = alpha0 * (m1 * r0 - t)
    direction = r1 + beta * r0
    along = alpha0 * (m1 * t - t2) + DAMPING * r1 + beta * (t + DAMPING * r0)
    parts = (alpha0 * r0, alpha1 * direction, r1, -alpha1 * along)
    for k, part in enumerate(parts):
        for c in range(3):
            out[k, c] = part[1 : 1 + CA, 1 : 1 + CB, c * CE : (c + 1) * CE]

    for copy, target in zip(halo + copies0 + copies1 + copies2, (has_up, has_down, has_right, has_left) + targets * 3):
        pl.when(target)(copy.wait_send)
    for stage in range(2):
        others = arr.at[stage, pl.ds(0, (ny if stage == 0 else nz) - 1)]
        pltpu.make_async_copy(others, others, ass.at[stage]).wait()


def solution(mesh):
    nz, ny = mesh.shape["gz"], mesh.shape["gy"]
    tables = constants()
    count = max(nz, ny)
    vmem = pltpu.VMEM
    dma = pltpu.SemaphoreType.DMA
    scratch = [
        vmem((CZ, CY, NX), F32), vmem((CZ, CY, NX), F32),
        vmem((CZ + 6, CY + 16, NX), F32),
        vmem((CZ, 8, NX), F32), vmem((CZ, 8, NX), F32), vmem((CZ, 8, NX), F32), vmem((CZ, 8, NX), F32),
        vmem((CZ, 4, NX), F32), vmem((CZ, 4, NX), F32),
        vmem((3, CY, NX), F32), vmem((3, CY, NX), F32),
        vmem((CZ, 4, NX), F32), vmem((CZ, 4, NX), F32),
        vmem((3, CZ, CY, NX), BF16),
        vmem((CZ * CY, NX), F32),
        vmem((CZ, CY, 2 * LANES), BF16),
        vmem((256, 3 * NX), BF16),
        vmem((ROWS, LANES), F32),
        vmem((A, B, LANES), F32),
        vmem((CZ, CY, LANES), F32),
        vmem((TABLE, NX), BF16),
        vmem((3, A, B, LANES), F32),
        vmem((3, 2, A, 4, LANES), F32),
        vmem((3, 2, 3, B, LANES), F32),
        vmem((3, 2, A, 4, LANES), F32),
        vmem((3, 4, 3, 4, LANES), F32),
        vmem((2, 4, LANES), F32),
        vmem((2, count, 4, LANES), F32),
        dma((12,)), dma((4,)), dma((4,)), dma((3, 8)), dma((3, 8)), dma((2,)), dma((2,)),
    ]
    out = jax.ShapeDtypeStruct((4, 3, CA, CB, CE), F32)
    call = pl.pallas_call(
        functools.partial(kernel, nz, ny),
        out_shape=out,
        in_specs=[pl.BlockSpec(memory_space=pl.ANY)] * 3,
        out_specs=pl.BlockSpec(memory_space=pltpu.VMEM),
        scratch_shapes=scratch,
        compiler_params=pltpu.CompilerParams(collective_id=0, has_side_effects=True, vmem_limit_bytes=VMEM_BYTES),
        name="cg_step",
    )

    def shards(fixed, moving):
        parts = call(fixed, moving, jnp.asarray(tables))
        return parts[0] + parts[1], parts[2] + parts[3]

    return jax.shard_map(
        shards,
        mesh=mesh,
        in_specs=(P("gz", "gy", None), P("gz", "gy", None)),
        out_specs=(P(None, "gz", "gy", None), P(None, "gz", "gy", None)),
        check_vma=False,
    )
```

```python
import functools

import jax
import jax.numpy as jnp
import numpy as np
from jax import lax
from jax.experimental import pallas as pl
from jax.experimental.pallas import tpu as pltpu
from jax.sharding import PartitionSpec as P

SPACING = 8
DAMPING = 8.0
CZ, CY, NX = 32, 64, 256
CA, CB, CE = 4, 8, 32
A, B, LANES = 7, 16, 128
BP = 11
ROWS = 80
DEEP = 8
CHUNK = DEEP * CY
INNER = 8
OUTER = 4
STRIPS = CZ * CY // NX
AT_BXE = NX
AT_BXD = AT_BXE + 3 * NX
AT_KE = AT_BXD + 6 * LANES
AT_KD = AT_KE + 2 * A * B * STRIPS
TABLE = AT_KD + CZ * CY
VMEM_BYTES = 52 * 1024 * 1024
MESH = pl.DeviceIdType.MESH
F32, BF16 = jnp.float32, jnp.bfloat16


def basis_matrix(count, columns, offset):
    voxel = np.arange(count)
    cell = voxel // SPACING
    frac = (voxel % SPACING + 0.5) / SPACING
    other = 1.0 - frac
    weights = (
        other**3 / 6.0,
        (3.0 * frac**3 - 6.0 * frac**2 + 4.0) / 6.0,
        (-3.0 * frac**3 + 3.0 * frac**2 + 3.0 * frac + 1.0) / 6.0,
        frac**3 / 6.0,
    )
    matrix = np.zeros((count, columns))
    for tap in range(4):
        for v in range(count):
            column = cell[v] - 1 + tap + offset
            if 0 <= column < columns:
                matrix[v, column] += weights[tap][v]
    return matrix


def halves(x):
    x = np.asarray(x, np.float32)
    high = x.astype(jnp.bfloat16)
    low = (x - high.astype(np.float32)).astype(jnp.bfloat16)
    return high, low


def constants():
    bz = basis_matrix(CZ, A, 1)
    by = basis_matrix(CY, B, 1)
    bx = basis_matrix(NX, CE, 0)
    narrow = np.einsum("za,yb->zyab", bz, by[:, :BP]).reshape(CZ * CY, A * BP)
    high, low = halves(np.pad(narrow, ((0, 0), (0, ROWS - A * BP))))
    pad = np.zeros((CZ * CY, 256 - 3 * ROWS), jnp.bfloat16)
    kd = np.concatenate([high, high, low, pad], axis=1)
    kron16 = np.einsum("za,yb->abzy", bz, by).reshape(A * B, CZ * CY)
    ke = np.concatenate(halves(kron16), axis=0)
    spread = np.zeros((LANES, 3 * NX))
    for c in range(3):
        spread[c * CE : (c + 1) * CE, c * NX : (c + 1) * NX] = bx.T
    high, low = halves(spread)
    bxd = np.concatenate([high, low], axis=0)
    bxe = np.concatenate([high.T, low.T], axis=1)
    dx = np.zeros((NX, NX))
    for step, weight in ((1, 45.0), (2, -9.0), (3, 1.0)):
        for v in range(NX):
            if v + step < NX:
                dx[v + step, v] = weight
            if v - step >= 0:
                dx[v - step, v] = -weight
    bxd = bxd.reshape(2 * LANES, 3, NX).transpose(1, 0, 2).reshape(6 * LANES, NX)
    ke = ke.reshape(2 * A * B, STRIPS, NX).transpose(1, 0, 2).reshape(2 * A * B * STRIPS, NX)
    return np.concatenate([dx.astype(jnp.bfloat16), bxe, bxd, ke, kd], axis=0)


def split(x):
    high = x.astype(BF16)
    return high, (x - high.astype(F32)).astype(BF16)


def dot(a, b):
    return jnp.dot(a, b, preferred_element_type=F32)


def kernel(nz, ny, fixed, moving, tab_h, out,
           fv, mv, mp, fl, ml, fh, mh, yls, yhs, zlr, zhr, ylr, yhr,
           g, along_s, u, cs, p3, tot, up_x, tab,
           enc, yst, rz, ry, rc, ars, arr,
           lsem, hss, hrs, xss, xrs, ass, arsem):
    d = lax.axis_index("gz")
    e = lax.axis_index("gy")
    up, down = lax.rem(d + 1, nz), lax.rem(d + nz - 1, nz)
    right, left = lax.rem(e + 1, ny), lax.rem(e + ny - 1, ny)

    has_down, has_up, has_left, has_right = d > 0, d < nz - 1, e > 0, e < ny - 1

    def local(k, src, dst):
        copy = pltpu.make_async_copy(src, dst, lsem.at[k])
        copy.start()
        return copy

    faces_z = [
        local(0, fixed.at[pl.ds(0, 3)], fv.at[pl.ds(0, 3)]),
        local(1, moving.at[pl.ds(0, 3)], mv.at[pl.ds(0, 3)]),
        local(2, fixed.at[pl.ds(CZ - 3, 3)], fv.at[pl.ds(CZ - 3, 3)]),
        local(3, moving.at[pl.ds(CZ - 3, 3)], mv.at[pl.ds(CZ - 3, 3)]),
    ]
    faces_y = [
        local(4, fixed.at[:, pl.ds(0, 8)], fl),
        local(5, moving.at[:, pl.ds(0, 8)], ml),
        local(6, fixed.at[:, pl.ds(CY - 8, 8)], fh),
        local(7, moving.at[:, pl.ds(CY - 8, 8)], mh),
    ]
    rest = [
        local(8, fixed.at[pl.ds(3, CZ - 6)], fv.at[pl.ds(3, CZ - 6)]),
        local(9, moving.at[pl.ds(3, CZ - 6)], mv.at[pl.ds(3, CZ - 6)]),
        local(10, tab_h.at[pl.ds(0, 4 * NX)], tab.at[pl.ds(0, 4 * NX)]),
    ]

    barrier = pltpu.get_barrier_semaphore()

    near = [(up, e), (down, e), (d, right), (d, left), (up, right), (up, left), (down, right), (down, left)]
    far = [(d, lax.rem(e + k, ny)) for k in range(2, ny - 1)] + [(lax.rem(d + k, nz), e) for k in range(2, nz - 1)]
    for target in near + far:
        pl.semaphore_signal(barrier, inc=1, device_id=target, device_id_type=MESH)

    def clear(missing, refs):
        @pl.when(jnp.logical_not(missing))
        def _():
            for ref in refs:
                ref[...] = jnp.zeros(ref.shape, F32)

    clear(has_down, [zlr] + [rz.at[k, 0] for k in range(3)])
    clear(has_up, [zhr] + [rz.at[k, 1] for k in range(3)])
    clear(has_left, [ylr] + [ry.at[k, 0] for k in range(3)])
    clear(has_right, [yhr] + [ry.at[k, 1] for k in range(3)])
    clear(has_down & has_left, [rc.at[k, 0] for k in range(3)])
    clear(has_down & has_right, [rc.at[k, 1] for k in range(3)])
    clear(has_up & has_left, [rc.at[k, 2] for k in range(3)])
    clear(has_up & has_right, [rc.at[k, 3] for k in range(3)])

    def remote(src, dst, send, recv, z, y):
        return pltpu.make_async_remote_copy(
            src_ref=src, dst_ref=dst, send_sem=send, recv_sem=recv, device_id=(z, y), device_id_type=MESH
        )

    for copy in faces_z:
        copy.wait()
    for z in (0, 1, 2, CZ - 3, CZ - 2, CZ - 1):
        mp[z + 3, 8 : 8 + CY, :] = 0.5 * (fv[z] + mv[z])
    pl.semaphore_wait(barrier, 4 + (ny - 1) + (nz - 1))
    halo = [
        remote(mp.at[pl.ds(CZ, 3), pl.ds(8, CY)], zlr, hss.at[0], hrs.at[0], up, e),
        remote(mp.at[pl.ds(3, 3), pl.ds(8, CY)], zhr, hss.at[1], hrs.at[1], down, e),
        remote(yhs, ylr, hss.at[2], hrs.at[2], d, right),
        remote(yls, yhr, hss.at[3], hrs.at[3], d, left),
    ]
    pl.when(has_up)(halo[0].start)
    pl.when(has_down)(halo[1].start)
    for copy in faces_y:
        copy.wait()
    yls[...] = 0.5 * (fl[:, 0:4, :] + ml[:, 0:4, :])
    yhs[...] = 0.5 * (fh[:, 4:8, :] + mh[:, 4:8, :])
    pl.when(has_right)(halo[2].start)
    pl.when(has_left)(halo[3].start)
    p3[...] = jnp.zeros_like(p3)
    cs[3 * ROWS : 256, :] = jnp.zeros((256 - 3 * ROWS, 3 * NX), BF16)

    for copy in rest:
        copy.wait()
    tail = pl.ds(4 * NX, TABLE - 4 * NX)
    later = [local(11, tab_h.at[tail], tab.at[tail])]

    def fill(z, carry):
        mp[z + 3, 8 : 8 + CY, :] = 0.5 * (fv[z] + mv[z])
        return carry

    lax.fori_loop(3, CZ - 3, fill, 0)

    def gather_x(volume):
        total = None
        for c in range(3):
            if volume[c] is None:
                continue
            term = dot(volume[c].astype(BF16), tab[AT_BXE + c * NX : AT_BXE + (c + 1) * NX, :])
            total = term if total is None else total + term
        return total[:, :LANES] + total[:, LANES:]

    edges, middle, every = ((0, 16), (CY - 16, 16)), ((16, CY - 32),), ((0, CY),)

    def first(z, layers, spans, parts, begun, done):
        count = layers * sum(size for unused, size in spans)
        deep = pl.ds(z, layers)

        def block(ref, dz, dy):
            pieces = [ref[pl.ds(z + dz, layers), dy + y : dy + y + size, :] for y, size in spans]
            whole = pieces[0] if len(pieces) == 1 else jnp.concatenate(pieces, axis=1)
            return whole.reshape(count, whole.shape[-1])

        def put(ref, value):
            value = value.reshape(layers, -1, value.shape[-1])
            at = 0
            for y, size in spans:
                ref[deep, y : y + size, :] = value[:, at : at + size]
                at += size

        def difference(part):
            return 45.0 * (part(1) - part(-1)) - 9.0 * (part(2) - part(-2)) + (part(3) - part(-3))

        mismatch = block(fv, 0, 0) - block(mv, 0, 0)
        volume = [None] * 3
        for c in parts:
            if c == 0:
                slope = difference(lambda k: block(mp, 3 + k, 8))
            elif c == 1:
                slope = difference(lambda k: block(mp, 3, 8 + k))
            else:
                high, low = split(block(mp, 3, 8))
                slope = dot(high, tab[0:NX, :]) + dot(low, tab[0:NX, :])
            rounded = (slope * (1.0 / 60.0)).astype(BF16)
            put(g.at[c], rounded)
            volume[c] = rounded.astype(F32) * mismatch
        total = gather_x(volume)
        if begun:
            total = total + block(up_x, 0, 0)
        if not done:
            put(up_x, total)
        else:
            high, low = split(total)
            put(u, jnp.concatenate([high, low], axis=1))

    inner, faces = (CZ - 2 * OUTER) // INNER, CZ - OUTER

    def own_inner(t, carry):
        first(OUTER + t * INNER, INNER, middle, (0, 1, 2), False, True)
        first(OUTER + t * INNER, INNER, edges, (0, 2), False, False)
        return carry

    def own_outer(t, carry):
        first(t * faces, OUTER, every, (2,), False, False)
        return carry

    def side_inner(t, carry):
        first(OUTER + t * INNER, INNER, edges, (1,), True, True)
        return carry

    def side_outer(t, carry):
        first(t * faces, OUTER, every, (1,), True, False)
        return carry

    def top_outer(t, carry):
        first(t * faces, OUTER, every, (0,), True, True)
        return carry

    lax.fori_loop(0, inner, own_inner, 0)
    lax.fori_loop(0, 2, own_outer, 0)
    pl.when(has_left)(halo[2].wait_recv)
    mp[3 : CZ + 3, 4:8, :] = ylr[...]
    pl.when(has_right)(halo[3].wait_recv)
    mp[3 : CZ + 3, 8 + CY : 12 + CY, :] = yhr[...]

    lax.fori_loop(0, inner, side_inner, 0)
    lax.fori_loop(0, 2, side_outer, 0)
    pl.when(has_down)(halo[0].wait_recv)
    mp[0:3, 8 : 8 + CY, :] = zlr[...]
    pl.when(has_up)(halo[1].wait_recv)
    mp[CZ + 3 : CZ + 6, 8 : 8 + CY, :] = zhr[...]
    lax.fori_loop(0, 2, top_outer, 0)
    for copy in later:
        copy.wait()

    row = lax.broadcasted_iota(jnp.int32, (1, 4, LANES), 1)
    low_rows = jnp.where(row < 3, 1.0, 0.0).astype(F32)
    pa = lax.broadcasted_iota(jnp.int32, (A, B, LANES), 0) + (d * CA - 1)
    pb = lax.broadcasted_iota(jnp.int32, (A, B, LANES), 1) + (e * CB - 1)
    ia = lax.broadcasted_iota(jnp.int32, (A, B, LANES), 0)
    ib = lax.broadcasted_iota(jnp.int32, (A, B, LANES), 1)
    inside = (pa >= 0) & (pa < nz * CA) & (pb >= 0) & (pb < ny * CB) & (ib < 11)
    inside = jnp.where(inside, 1.0, 0.0).astype(F32)
    own = jnp.where((ia >= 1) & (ia < 1 + CA) & (ib >= 1) & (ib < 1 + CB), 1.0, 0.0).astype(F32)

    targets = (has_up & has_right, has_up & has_left, has_down & has_right, has_down & has_left,
               has_up, has_down, has_right, has_left)
    sources = (has_down & has_left, has_down & has_right, has_up & has_left, has_up & has_right,
               has_down, has_up, has_left, has_right)

    def exchange(k):
        half = A * B
        both = None
        for n in range(STRIPS):
            strip = tab[AT_KE + n * 2 * half : AT_KE + (n + 1) * 2 * half, :]
            layers = NX // CY
            term = dot(strip, u[n * layers : (n + 1) * layers].reshape(NX, 2 * LANES))
            both = term if both is None else both + term
        total = both[:half, :LANES] + both[half:, :LANES] + both[:half, LANES:]
        total = total.reshape(A, B, LANES)
        enc[k] = total
        yst[k, 0] = total[:, 8:12]
        yst[k, 1] = total[:, 0:4]
        src, after, before = enc.at[k], yst.at[k, 0], yst.at[k, 1]
        top, bottom = pl.ds(A - 3, 3), pl.ds(0, 3)
        copies = [
            remote(after.at[top], rc.at[k, 0], xss.at[k, 0], xrs.at[k, 0], up, right),
            remote(before.at[top], rc.at[k, 1], xss.at[k, 1], xrs.at[k, 1], up, left),
            remote(after.at[bottom], rc.at[k, 2], xss.at[k, 2], xrs.at[k, 2], down, right),
            remote(before.at[bottom], rc.at[k, 3], xss.at[k, 3], xrs.at[k, 3], down, left),
            remote(src.at[top], rz.at[k, 0], xss.at[k, 4], xrs.at[k, 4], up, e),
            remote(src.at[bottom], rz.at[k, 1], xss.at[k, 5], xrs.at[k, 5], down, e),
            remote(after, ry.at[k, 0], xss.at[k, 6], xrs.at[k, 6], d, right),
            remote(before, ry.at[k, 1], xss.at[k, 7], xrs.at[k, 7], d, left),
        ]
        for copy, target in zip(copies, targets):
            pl.when(target)(copy.start)
        return copies

    def collect(k, copies):
        tot[...] = enc[k]
        for n in (7, 6, 5, 4):
            pl.when(sources[n])(copies[n].wait_recv)
        tot[:, 0:4] += ry[k, 0]
        tot[:, 8:12] += low_rows * ry[k, 1]
        tot[0:3] += rz[k, 0]
        tot[4:7] += rz[k, 1]
        for n in range(4):
            pl.when(sources[n])(copies[n].wait_recv)
        tot[0:3, 0:4] += rc[k, 0]
        tot[0:3, 8:12] += low_rows * rc[k, 1]
        tot[4:7, 0:4] += rc[k, 2]
        tot[4:7, 8:12] += low_rows * rc[k, 3]
        return tot[...] * inside

    def spread_x(control):
        for a in range(A):
            p3[a * BP : (a + 1) * BP, :] = control[a, 0:BP, :]
        high, low = split(p3[...])
        twice = jnp.concatenate([high, high], axis=1)
        wide = []
        for c in range(3):
            at = AT_BXD + c * 2 * LANES
            wide.append(dot(twice, tab[at : at + 2 * LANES, :]) + dot(low, tab[at : at + LANES, :]))
        high, low = split(jnp.concatenate(wide, axis=1))
        cs[0:ROWS, :] = high
        cs[ROWS : 2 * ROWS, :] = low
        cs[2 * ROWS : 3 * ROWS, :] = high

    def strip_of(i):
        return slice(i * DEEP, (i + 1) * DEEP), slice(i * CHUNK, (i + 1) * CHUNK)

    def decode(i):
        unused, rows = strip_of(i)
        weights = tab[AT_KD + i * CHUNK : AT_KD + (i + 1) * CHUNK, :]
        return [dot(weights, cs[:, c * NX : (c + 1) * NX]) for c in range(3)]

    def slopes_of(i):
        deep, unused = strip_of(i)
        return [g[c, deep].reshape(CHUNK, NX).astype(F32) for c in range(3)]

    def along(i):
        field, slopes = decode(i), slopes_of(i)
        s = slopes[0] * field[0] + slopes[1] * field[1] + slopes[2] * field[2]
        return slopes, s, jnp.sum((s * s).reshape(CHUNK // 8, 8, NX), axis=0)

    def keep(i, slopes, s):
        deep, unused = strip_of(i)
        high, low = split(gather_x([slopes[c] * s for c in range(3)]))
        u[deep] = jnp.concatenate([high, low], axis=1).reshape(DEEP, CY, 2 * LANES)

    def apply():
        total = jnp.zeros((8, NX), F32)
        for i in range(CZ // DEEP):
            slopes, s, square = along(i)
            keep(i, slopes, s)
            total = total + square
        return fold(total)

    def apply_forward():
        total = jnp.zeros((8, NX), F32)
        for i in range(CZ // DEEP):
            unused, rows = strip_of(i)
            unused, s, square = along(i)
            along_s[rows, :] = s
            total = total + square
        return fold(total)

    def apply_back():
        for i in range(CZ // DEEP):
            unused, rows = strip_of(i)
            keep(i, slopes_of(i), along_s[rows, :])

    def fold(x):
        total = jnp.sum(x, axis=0, keepdims=True)
        return total[:, 0:LANES] + total[:, LANES : 2 * LANES]

    def tile_sum(x):
        return jnp.sum(jnp.sum(x, axis=0), axis=0, keepdims=True)

    def reduce_start(stage, value):
        me, count = (e, ny) if stage == 0 else (d, nz)
        ars[stage] = value
        arr[stage, me] = value

        for k in sorted(range(1, count), key=lambda k: -min(k, count - k)):
            other = lax.rem(me + k, count)
            z, y = (d, other) if stage == 0 else (other, e)
            remote(ars.at[stage], arr.at[stage, me], ass.at[stage], arsem.at[stage], z, y).start()

    def reduce_end(stage):
        count = ny if stage == 0 else nz
        others = arr.at[stage, pl.ds(0, count - 1)]
        pltpu.make_async_copy(others, others, arsem.at[stage]).wait()
        return jnp.sum(arr[stage, 0:count], axis=0)

    copies0 = exchange(0)
    r0 = collect(0, copies0)
    spread_x(r0)
    square0 = tile_sum(r0 * r0 * own)
    energy0 = apply()
    copies1 = exchange(1)
    t = collect(1, copies1)
    spread_x(t)
    square1 = tile_sum(t * t * own)
    sums = [square0, energy0, square1, apply_forward()]
    reduce_start(0, jnp.concatenate(sums, axis=0))
    apply_back()
    copies2 = exchange(2)
    reduce_start(1, reduce_end(0))
    t2 = collect(2, copies2)
    total = jnp.sum(reduce_end(1), axis=1, keepdims=True)
    rr0 = total[0:1]
    m1, m2, m3 = (total[k : k + 1] / rr0 for k in (1, 2, 3))
    alpha0 = 1.0 / (m1 + DAMPING)
    beta = alpha0 * alpha0 * (m2 - m1 * m1)
    curve = alpha0 * alpha0 * ((m3 - m1 * m2) - m1 * (m2 - m1 * m1)) + DAMPING * beta
    alpha1 = beta / (curve - beta * beta / alpha0)
    m1, alpha0, alpha1, beta = (x.reshape(1, 1, 1) for x in (m1, alpha0, alpha1, beta))
    r1 = alpha0 * (m1 * r0 - t)
    direction = r1 + beta * r0
    along = alpha0 * (m1 * t - t2) + DAMPING * r1 + beta * (t + DAMPING * r0)
    parts = (alpha0 * r0, alpha1 * direction, r1, -alpha1 * along)
    for k, part in enumerate(parts):
        for c in range(3):
            out[k, c] = part[1 : 1 + CA, 1 : 1 + CB, c * CE : (c + 1) * CE]

    for copy, target in zip(halo + copies0 + copies1 + copies2, (has_up, has_down, has_right, has_left) + targets * 3):
        pl.when(target)(copy.wait_send)
    for stage in range(2):
        others = arr.at[stage, pl.ds(0, (ny if stage == 0 else nz) - 1)]
        pltpu.make_async_copy(others, others, ass.at[stage]).wait()


def solution(mesh):
    nz, ny = mesh.shape["gz"], mesh.shape["gy"]
    tables = constants()
    count = max(nz, ny)
    vmem = pltpu.VMEM
    dma = pltpu.SemaphoreType.DMA
    scratch = [
        vmem((CZ, CY, NX), F32), vmem((CZ, CY, NX), F32),
        vmem((CZ + 6, CY + 16, NX), F32),
        vmem((CZ, 8, NX), F32), vmem((CZ, 8, NX), F32), vmem((CZ, 8, NX), F32), vmem((CZ, 8, NX), F32),
        vmem((CZ, 4, NX), F32), vmem((CZ, 4, NX), F32),
        vmem((3, CY, NX), F32), vmem((3, CY, NX), F32),
        vmem((CZ, 4, NX), F32), vmem((CZ, 4, NX), F32),
        vmem((3, CZ, CY, NX), BF16),
        vmem((CZ * CY, NX), F32),
        vmem((CZ, CY, 2 * LANES), BF16),
        vmem((256, 3 * NX), BF16),
        vmem((ROWS, LANES), F32),
        vmem((A, B, LANES), F32),
        vmem((CZ, CY, LANES), F32),
        vmem((TABLE, NX), BF16),
        vmem((3, A, B, LANES), F32),
        vmem((3, 2, A, 4, LANES), F32),
        vmem((3, 2, 3, B, LANES), F32),
        vmem((3, 2, A, 4, LANES), F32),
        vmem((3, 4, 3, 4, LANES), F32),
        vmem((2, 4, LANES), F32),
        vmem((2, count, 4, LANES), F32),
        dma((12,)), dma((4,)), dma((4,)), dma((3, 8)), dma((3, 8)), dma((2,)), dma((2,)),
    ]
    out = jax.ShapeDtypeStruct((4, 3, CA, CB, CE), F32)
    call = pl.pallas_call(
        functools.partial(kernel, nz, ny),
        out_shape=out,
        in_specs=[pl.BlockSpec(memory_space=pl.ANY)] * 3,
        out_specs=pl.BlockSpec(memory_space=pltpu.VMEM),
        scratch_shapes=scratch,
        compiler_params=pltpu.CompilerParams(collective_id=0, has_side_effects=True, vmem_limit_bytes=VMEM_BYTES),
        name="cg_step",
    )

    def shards(fixed, moving):
        parts = call(fixed, moving, jnp.asarray(tables))
        return parts[0] + parts[1], parts[2] + parts[3]

    return jax.shard_map(
        shards,
        mesh=mesh,
        in_specs=(P("gz", "gy", None), P("gz", "gy", None)),
        out_specs=(P(None, "gz", "gy", None), P(None, "gz", "gy", None)),
        check_vma=False,
    )
```

```python
import functools

import jax
import jax.numpy as jnp
import numpy as np
from jax import lax
from jax.experimental import pallas as pl
from jax.experimental.pallas import tpu as pltpu
from jax.sharding import PartitionSpec as P

SPACING = 8
DAMPING = 8.0
CZ, CY, NX = 32, 64, 256
CA, CB, CE = 4, 8, 32
A, B, LANES = 7, 16, 128
BP = 11
ROWS = 80
DEEP = 8
CHUNK = DEEP * CY
INNER = 8
OUTER = 4
STRIPS = CZ * CY // NX
AT_BXE = NX
AT_BXD = AT_BXE + 3 * NX
AT_KE = AT_BXD + 6 * LANES
AT_KD = AT_KE + 2 * A * B * STRIPS
TABLE = AT_KD + CZ * CY
VMEM_BYTES = 52 * 1024 * 1024
MESH = pl.DeviceIdType.MESH
F32, BF16 = jnp.float32, jnp.bfloat16


def basis_matrix(count, columns, offset):
    voxel = np.arange(count)
    cell = voxel // SPACING
    frac = (voxel % SPACING + 0.5) / SPACING
    other = 1.0 - frac
    weights = (
        other**3 / 6.0,
        (3.0 * frac**3 - 6.0 * frac**2 + 4.0) / 6.0,
        (-3.0 * frac**3 + 3.0 * frac**2 + 3.0 * frac + 1.0) / 6.0,
        frac**3 / 6.0,
    )
    matrix = np.zeros((count, columns))
    for tap in range(4):
        for v in range(count):
            column = cell[v] - 1 + tap + offset
            if 0 <= column < columns:
                matrix[v, column] += weights[tap][v]
    return matrix


def halves(x):
    x = np.asarray(x, np.float32)
    high = x.astype(jnp.bfloat16)
    low = (x - high.astype(np.float32)).astype(jnp.bfloat16)
    return high, low


def constants():
    bz = basis_matrix(CZ, A, 1)
    by = basis_matrix(CY, B, 1)
    bx = basis_matrix(NX, CE, 0)
    narrow = np.einsum("za,yb->zyab", bz, by[:, :BP]).reshape(CZ * CY, A * BP)
    high, low = halves(np.pad(narrow, ((0, 0), (0, ROWS - A * BP))))
    pad = np.zeros((CZ * CY, 256 - 3 * ROWS), jnp.bfloat16)
    kd = np.concatenate([high, high, low, pad], axis=1)
    kron16 = np.einsum("za,yb->abzy", bz, by).reshape(A * B, CZ * CY)
    ke = np.concatenate(halves(kron16), axis=0)
    spread = np.zeros((LANES, 3 * NX))
    for c in range(3):
        spread[c * CE : (c + 1) * CE, c * NX : (c + 1) * NX] = bx.T
    high, low = halves(spread)
    bxd = np.concatenate([high, low], axis=0)
    bxe = np.concatenate([high.T, low.T], axis=1)
    dx = np.zeros((NX, NX))
    for step, weight in ((1, 45.0), (2, -9.0), (3, 1.0)):
        for v in range(NX):
            if v + step < NX:
                dx[v + step, v] = weight
            if v - step >= 0:
                dx[v - step, v] = -weight
    bxd = bxd.reshape(2 * LANES, 3, NX).transpose(1, 0, 2).reshape(6 * LANES, NX)
    ke = ke.reshape(2 * A * B, STRIPS, NX).transpose(1, 0, 2).reshape(2 * A * B * STRIPS, NX)
    return np.concatenate([dx.astype(jnp.bfloat16), bxe, bxd, ke, kd], axis=0)


def split(x):
    high = x.astype(BF16)
    return high, (x - high.astype(F32)).astype(BF16)


def dot(a, b):
    return jnp.dot(a, b, preferred_element_type=F32)


def kernel(nz, ny, fixed, moving, tab_h, out,
           fv, mv, mp, fl, ml, fh, mh, yls, yhs, zlr, zhr, ylr, yhr,
           g, along_s, u, cs, p3, tot, up_x, tab,
           enc, yst, rz, ry, rc, ars, arr,
           lsem, hss, hrs, xss, xrs, ass, arsem):
    d = lax.axis_index("gz")
    e = lax.axis_index("gy")
    up, down = lax.rem(d + 1, nz), lax.rem(d + nz - 1, nz)
    right, left = lax.rem(e + 1, ny), lax.rem(e + ny - 1, ny)

    has_down, has_up, has_left, has_right = d > 0, d < nz - 1, e > 0, e < ny - 1

    def local(k, src, dst):
        copy = pltpu.make_async_copy(src, dst, lsem.at[k])
        copy.start()
        return copy

    faces_z = [
        local(0, fixed.at[pl.ds(0, 3)], fv.at[pl.ds(0, 3)]),
        local(1, moving.at[pl.ds(0, 3)], mv.at[pl.ds(0, 3)]),
        local(2, fixed.at[pl.ds(CZ - 3, 3)], fv.at[pl.ds(CZ - 3, 3)]),
        local(3, moving.at[pl.ds(CZ - 3, 3)], mv.at[pl.ds(CZ - 3, 3)]),
    ]
    faces_y = [
        local(4, fixed.at[:, pl.ds(0, 8)], fl),
        local(5, moving.at[:, pl.ds(0, 8)], ml),
        local(6, fixed.at[:, pl.ds(CY - 8, 8)], fh),
        local(7, moving.at[:, pl.ds(CY - 8, 8)], mh),
    ]
    rest = [
        local(8, fixed.at[pl.ds(3, CZ - 6)], fv.at[pl.ds(3, CZ - 6)]),
        local(9, moving.at[pl.ds(3, CZ - 6)], mv.at[pl.ds(3, CZ - 6)]),
        local(10, tab_h.at[pl.ds(0, 4 * NX)], tab.at[pl.ds(0, 4 * NX)]),
    ]

    barrier = pltpu.get_barrier_semaphore()

    near = [(up, e), (down, e), (d, right), (d, left), (up, right), (up, left), (down, right), (down, left)]
    far = [(d, lax.rem(e + k, ny)) for k in range(2, ny - 1)] + [(lax.rem(d + k, nz), e) for k in range(2, nz - 1)]
    for target in near + far:
        pl.semaphore_signal(barrier, inc=1, device_id=target, device_id_type=MESH)

    def clear(missing, refs):
        @pl.when(jnp.logical_not(missing))
        def _():
            for ref in refs:
                ref[...] = jnp.zeros(ref.shape, F32)

    clear(has_down, [zlr] + [rz.at[k, 0] for k in range(3)])
    clear(has_up, [zhr] + [rz.at[k, 1] for k in range(3)])
    clear(has_left, [ylr] + [ry.at[k, 0] for k in range(3)])
    clear(has_right, [yhr] + [ry.at[k, 1] for k in range(3)])
    clear(has_down & has_left, [rc.at[k, 0] for k in range(3)])
    clear(has_down & has_right, [rc.at[k, 1] for k in range(3)])
    clear(has_up & has_left, [rc.at[k, 2] for k in range(3)])
    clear(has_up & has_right, [rc.at[k, 3] for k in range(3)])

    def remote(src, dst, send, recv, z, y):
        return pltpu.make_async_remote_copy(
            src_ref=src, dst_ref=dst, send_sem=send, recv_sem=recv, device_id=(z, y), device_id_type=MESH
        )

    for copy in faces_z:
        copy.wait()
    for z in (0, 1, 2, CZ - 3, CZ - 2, CZ - 1):
        mp[z + 3, 8 : 8 + CY, :] = 0.5 * (fv[z] + mv[z])
    pl.semaphore_wait(barrier, 4 + (ny - 1) + (nz - 1))
    halo = [
        remote(mp.at[pl.ds(CZ, 3), pl.ds(8, CY)], zlr, hss.at[0], hrs.at[0], up, e),
        remote(mp.at[pl.ds(3, 3), pl.ds(8, CY)], zhr, hss.at[1], hrs.at[1], down, e),
        remote(yhs, ylr, hss.at[2], hrs.at[2], d, right),
        remote(yls, yhr, hss.at[3], hrs.at[3], d, left),
    ]
    pl.when(has_up)(halo[0].start)
    pl.when(has_down)(halo[1].start)
    for copy in faces_y:
        copy.wait()
    yls[...] = 0.5 * (fl[:, 0:4, :] + ml[:, 0:4, :])
    yhs[...] = 0.5 * (fh[:, 4:8, :] + mh[:, 4:8, :])
    pl.when(has_right)(halo[2].start)
    pl.when(has_left)(halo[3].start)
    p3[...] = jnp.zeros_like(p3)
    cs[3 * ROWS : 256, :] = jnp.zeros((256 - 3 * ROWS, 3 * NX), BF16)

    for copy in rest:
        copy.wait()
    tail = pl.ds(4 * NX, TABLE - 4 * NX)
    later = [local(11, tab_h.at[tail], tab.at[tail])]

    def fill(z, carry):
        mp[z + 3, 8 : 8 + CY, :] = 0.5 * (fv[z] + mv[z])
        return carry

    lax.fori_loop(3, CZ - 3, fill, 0)

    def gather_x(volume):
        total = None
        for c in range(3):
            if volume[c] is None:
                continue
            term = dot(volume[c].astype(BF16), tab[AT_BXE + c * NX : AT_BXE + (c + 1) * NX, :])
            total = term if total is None else total + term
        return total[:, :LANES] + total[:, LANES:]

    edges, middle, every = ((0, 16), (CY - 16, 16)), ((16, CY - 32),), ((0, CY),)

    def first(z, layers, spans, parts, begun, done):
        count = layers * sum(size for unused, size in spans)
        deep = pl.ds(z, layers)

        def block(ref, dz, dy):
            pieces = [ref[pl.ds(z + dz, layers), dy + y : dy + y + size, :] for y, size in spans]
            whole = pieces[0] if len(pieces) == 1 else jnp.concatenate(pieces, axis=1)
            return whole.reshape(count, whole.shape[-1])

        def put(ref, value):
            value = value.reshape(layers, -1, value.shape[-1])
            at = 0
            for y, size in spans:
                ref[deep, y : y + size, :] = value[:, at : at + size]
                at += size

        def difference(part):
            return 45.0 * (part(1) - part(-1)) - 9.0 * (part(2) - part(-2)) + (part(3) - part(-3))

        mismatch = block(fv, 0, 0) - block(mv, 0, 0)
        volume = [None] * 3
        for c in parts:
            if c == 0:
                slope = difference(lambda k: block(mp, 3 + k, 8))
            elif c == 1:
                slope = difference(lambda k: block(mp, 3, 8 + k))
            else:
                high, low = split(block(mp, 3, 8))
                slope = dot(high, tab[0:NX, :]) + dot(low, tab[0:NX, :])
            rounded = (slope * (1.0 / 60.0)).astype(BF16)
            put(g.at[c], rounded)
            volume[c] = rounded.astype(F32) * mismatch
        total = gather_x(volume)
        if begun:
            total = total + block(up_x, 0, 0)
        if not done:
            put(up_x, total)
        else:
            high, low = split(total)
            put(u, jnp.concatenate([high, low], axis=1))

    inner, faces = (CZ - 2 * OUTER) // INNER, CZ - OUTER

    def own_inner(t, carry):
        first(OUTER + t * INNER, INNER, middle, (0, 1, 2), False, True)
        first(OUTER + t * INNER, INNER, edges, (0, 2), False, False)
        return carry

    def own_outer(t, carry):
        first(t * faces, OUTER, every, (2,), False, False)
        return carry

    def side_inner(t, carry):
        first(OUTER + t * INNER, INNER, edges, (1,), True, True)
        return carry

    def side_outer(t, carry):
        first(t * faces, OUTER, every, (1,), True, False)
        return carry

    def top_outer(t, carry):
        first(t * faces, OUTER, every, (0,), True, True)
        return carry

    lax.fori_loop(0, inner, own_inner, 0)
    lax.fori_loop(0, 2, own_outer, 0)
    pl.when(has_left)(halo[2].wait_recv)
    mp[3 : CZ + 3, 4:8, :] = ylr[...]
    pl.when(has_right)(halo[3].wait_recv)
    mp[3 : CZ + 3, 8 + CY : 12 + CY, :] = yhr[...]

    for t in range(inner):
        side_inner(t, 0)
    for t in range(2):
        side_outer(t, 0)
    pl.when(has_down)(halo[0].wait_recv)
    mp[0:3, 8 : 8 + CY, :] = zlr[...]
    pl.when(has_up)(halo[1].wait_recv)
    mp[CZ + 3 : CZ + 6, 8 : 8 + CY, :] = zhr[...]
    for t in range(2):
        top_outer(t, 0)
    for copy in later:
        copy.wait()

    row = lax.broadcasted_iota(jnp.int32, (1, 4, LANES), 1)
    low_rows = jnp.where(row < 3, 1.0, 0.0).astype(F32)
    pa = lax.broadcasted_iota(jnp.int32, (A, B, LANES), 0) + (d * CA - 1)
    pb = lax.broadcasted_iota(jnp.int32, (A, B, LANES), 1) + (e * CB - 1)
    ia = lax.broadcasted_iota(jnp.int32, (A, B, LANES), 0)
    ib = lax.broadcasted_iota(jnp.int32, (A, B, LANES), 1)
    inside = (pa >= 0) & (pa < nz * CA) & (pb >= 0) & (pb < ny * CB) & (ib < 11)
    inside = jnp.where(inside, 1.0, 0.0).astype(F32)
    own = jnp.where((ia >= 1) & (ia < 1 + CA) & (ib >= 1) & (ib < 1 + CB), 1.0, 0.0).astype(F32)

    targets = (has_up & has_right, has_up & has_left, has_down & has_right, has_down & has_left,
               has_up, has_down, has_right, has_left)
    sources = (has_down & has_left, has_down & has_right, has_up & has_left, has_up & has_right,
               has_down, has_up, has_left, has_right)

    def exchange(k):
        half = A * B
        both = None
        for n in range(STRIPS):
            strip = tab[AT_KE + n * 2 * half : AT_KE + (n + 1) * 2 * half, :]
            layers = NX // CY
            term = dot(strip, u[n * layers : (n + 1) * layers].reshape(NX, 2 * LANES))
            both = term if both is None else both + term
        total = both[:half, :LANES] + both[half:, :LANES] + both[:half, LANES:]
        total = total.reshape(A, B, LANES)
        enc[k] = total
        yst[k, 0] = total[:, 8:12]
        yst[k, 1] = total[:, 0:4]
        src, after, before = enc.at[k], yst.at[k, 0], yst.at[k, 1]
        top, bottom = pl.ds(A - 3, 3), pl.ds(0, 3)
        copies = [
            remote(after.at[top], rc.at[k, 0], xss.at[k, 0], xrs.at[k, 0], up, right),
            remote(before.at[top], rc.at[k, 1], xss.at[k, 1], xrs.at[k, 1], up, left),
            remote(after.at[bottom], rc.at[k, 2], xss.at[k, 2], xrs.at[k, 2], down, right),
            remote(before.at[bottom], rc.at[k, 3], xss.at[k, 3], xrs.at[k, 3], down, left),
            remote(src.at[top], rz.at[k, 0], xss.at[k, 4], xrs.at[k, 4], up, e),
            remote(src.at[bottom], rz.at[k, 1], xss.at[k, 5], xrs.at[k, 5], down, e),
            remote(after, ry.at[k, 0], xss.at[k, 6], xrs.at[k, 6], d, right),
            remote(before, ry.at[k, 1], xss.at[k, 7], xrs.at[k, 7], d, left),
        ]
        for copy, target in zip(copies, targets):
            pl.when(target)(copy.start)
        return copies

    def collect(k, copies):
        tot[...] = enc[k]
        for n in (7, 6, 5, 4):
            pl.when(sources[n])(copies[n].wait_recv)
        tot[:, 0:4] += ry[k, 0]
        tot[:, 8:12] += low_rows * ry[k, 1]
        tot[0:3] += rz[k, 0]
        tot[4:7] += rz[k, 1]
        for n in range(4):
            pl.when(sources[n])(copies[n].wait_recv)
        tot[0:3, 0:4] += rc[k, 0]
        tot[0:3, 8:12] += low_rows * rc[k, 1]
        tot[4:7, 0:4] += rc[k, 2]
        tot[4:7, 8:12] += low_rows * rc[k, 3]
        return tot[...] * inside

    def spread_x(control):
        for a in range(A):
            p3[a * BP : (a + 1) * BP, :] = control[a, 0:BP, :]
        high, low = split(p3[...])
        twice = jnp.concatenate([high, high], axis=1)
        wide = []
        for c in range(3):
            at = AT_BXD + c * 2 * LANES
            wide.append(dot(twice, tab[at : at + 2 * LANES, :]) + dot(low, tab[at : at + LANES, :]))
        high, low = split(jnp.concatenate(wide, axis=1))
        cs[0:ROWS, :] = high
        cs[ROWS : 2 * ROWS, :] = low
        cs[2 * ROWS : 3 * ROWS, :] = high

    def strip_of(i):
        return slice(i * DEEP, (i + 1) * DEEP), slice(i * CHUNK, (i + 1) * CHUNK)

    def decode(i):
        unused, rows = strip_of(i)
        weights = tab[AT_KD + i * CHUNK : AT_KD + (i + 1) * CHUNK, :]
        return [dot(weights, cs[:, c * NX : (c + 1) * NX]) for c in range(3)]

    def slopes_of(i):
        deep, unused = strip_of(i)
        return [g[c, deep].reshape(CHUNK, NX).astype(F32) for c in range(3)]

    def along(i):
        field, slopes = decode(i), slopes_of(i)
        s = slopes[0] * field[0] + slopes[1] * field[1] + slopes[2] * field[2]
        return slopes, s, jnp.sum((s * s).reshape(CHUNK // 8, 8, NX), axis=0)

    def keep(i, slopes, s):
        deep, unused = strip_of(i)
        high, low = split(gather_x([slopes[c] * s for c in range(3)]))
        u[deep] = jnp.concatenate([high, low], axis=1).reshape(DEEP, CY, 2 * LANES)

    def apply():
        total = jnp.zeros((8, NX), F32)
        for i in range(CZ // DEEP):
            slopes, s, square = along(i)
            keep(i, slopes, s)
            total = total + square
        return fold(total)

    def apply_forward():
        total = jnp.zeros((8, NX), F32)
        for i in range(CZ // DEEP):
            unused, rows = strip_of(i)
            unused, s, square = along(i)
            along_s[rows, :] = s
            total = total + square
        return fold(total)

    def apply_back():
        for i in range(CZ // DEEP):
            unused, rows = strip_of(i)
            keep(i, slopes_of(i), along_s[rows, :])

    def fold(x):
        total = jnp.sum(x, axis=0, keepdims=True)
        return total[:, 0:LANES] + total[:, LANES : 2 * LANES]

    def tile_sum(x):
        return jnp.sum(jnp.sum(x, axis=0), axis=0, keepdims=True)

    def reduce_start(stage, value):
        me, count = (e, ny) if stage == 0 else (d, nz)
        ars[stage] = value
        arr[stage, me] = value

        for k in sorted(range(1, count), key=lambda k: -min(k, count - k)):
            other = lax.rem(me + k, count)
            z, y = (d, other) if stage == 0 else (other, e)
            remote(ars.at[stage], arr.at[stage, me], ass.at[stage], arsem.at[stage], z, y).start()

    def reduce_end(stage):
        count = ny if stage == 0 else nz
        others = arr.at[stage, pl.ds(0, count - 1)]
        pltpu.make_async_copy(others, others, arsem.at[stage]).wait()
        return jnp.sum(arr[stage, 0:count], axis=0)

    copies0 = exchange(0)
    r0 = collect(0, copies0)
    spread_x(r0)
    square0 = tile_sum(r0 * r0 * own)
    energy0 = apply()
    copies1 = exchange(1)
    t = collect(1, copies1)
    spread_x(t)
    square1 = tile_sum(t * t * own)
    sums = [square0, energy0, square1, apply_forward()]
    reduce_start(0, jnp.concatenate(sums, axis=0))
    apply_back()
    copies2 = exchange(2)
    reduce_start(1, reduce_end(0))
    t2 = collect(2, copies2)
    total = jnp.sum(reduce_end(1), axis=1, keepdims=True)
    rr0 = total[0:1]
    m1, m2, m3 = (total[k : k + 1] / rr0 for k in (1, 2, 3))
    alpha0 = 1.0 / (m1 + DAMPING)
    beta = alpha0 * alpha0 * (m2 - m1 * m1)
    curve = alpha0 * alpha0 * ((m3 - m1 * m2) - m1 * (m2 - m1 * m1)) + DAMPING * beta
    alpha1 = beta / (curve - beta * beta / alpha0)
    m1, alpha0, alpha1, beta = (x.reshape(1, 1, 1) for x in (m1, alpha0, alpha1, beta))
    r1 = alpha0 * (m1 * r0 - t)
    direction = r1 + beta * r0
    along = alpha0 * (m1 * t - t2) + DAMPING * r1 + beta * (t + DAMPING * r0)
    parts = (alpha0 * r0, alpha1 * direction, r1, -alpha1 * along)
    for k, part in enumerate(parts):
        for c in range(3):
            out[k, c] = part[1 : 1 + CA, 1 : 1 + CB, c * CE : (c + 1) * CE]

    for copy, target in zip(halo + copies0 + copies1 + copies2, (has_up, has_down, has_right, has_left) + targets * 3):
        pl.when(target)(copy.wait_send)
    for stage in range(2):
        others = arr.at[stage, pl.ds(0, (ny if stage == 0 else nz) - 1)]
        pltpu.make_async_copy(others, others, ass.at[stage]).wait()


def solution(mesh):
    nz, ny = mesh.shape["gz"], mesh.shape["gy"]
    tables = constants()
    count = max(nz, ny)
    vmem = pltpu.VMEM
    dma = pltpu.SemaphoreType.DMA
    scratch = [
        vmem((CZ, CY, NX), F32), vmem((CZ, CY, NX), F32),
        vmem((CZ + 6, CY + 16, NX), F32),
        vmem((CZ, 8, NX), F32), vmem((CZ, 8, NX), F32), vmem((CZ, 8, NX), F32), vmem((CZ, 8, NX), F32),
        vmem((CZ, 4, NX), F32), vmem((CZ, 4, NX), F32),
        vmem((3, CY, NX), F32), vmem((3, CY, NX), F32),
        vmem((CZ, 4, NX), F32), vmem((CZ, 4, NX), F32),
        vmem((3, CZ, CY, NX), BF16),
        vmem((CZ * CY, NX), F32),
        vmem((CZ, CY, 2 * LANES), BF16),
        vmem((256, 3 * NX), BF16),
        vmem((ROWS, LANES), F32),
        vmem((A, B, LANES), F32),
        vmem((CZ, CY, LANES), F32),
        vmem((TABLE, NX), BF16),
        vmem((3, A, B, LANES), F32),
        vmem((3, 2, A, 4, LANES), F32),
        vmem((3, 2, 3, B, LANES), F32),
        vmem((3, 2, A, 4, LANES), F32),
        vmem((3, 4, 3, 4, LANES), F32),
        vmem((2, 4, LANES), F32),
        vmem((2, count, 4, LANES), F32),
        dma((12,)), dma((4,)), dma((4,)), dma((3, 8)), dma((3, 8)), dma((2,)), dma((2,)),
    ]
    out = jax.ShapeDtypeStruct((4, 3, CA, CB, CE), F32)
    call = pl.pallas_call(
        functools.partial(kernel, nz, ny),
        out_shape=out,
        in_specs=[pl.BlockSpec(memory_space=pl.ANY)] * 3,
        out_specs=pl.BlockSpec(memory_space=pltpu.VMEM),
        scratch_shapes=scratch,
        compiler_params=pltpu.CompilerParams(collective_id=0, has_side_effects=True, vmem_limit_bytes=VMEM_BYTES),
        name="cg_step",
    )

    def shards(fixed, moving):
        parts = call(fixed, moving, jnp.asarray(tables))
        return parts[0] + parts[1], parts[2] + parts[3]

    return jax.shard_map(
        shards,
        mesh=mesh,
        in_specs=(P("gz", "gy", None), P("gz", "gy", None)),
        out_specs=(P(None, "gz", "gy", None), P(None, "gz", "gy", None)),
        check_vma=False,
    )
```
